32 devices in a mesh: seq: 8 (over z, y), head: 4 (over x, core).
Axes of the slice: x: 2, y: 2, z: 4, core: 2. Of those that a mesh axis runs over, the one named last changes fastest.
Arguments:
- queries: bfloat16 [1024, 4096], P('seq', 'head'), may hold values from -12 to 12
- keys: bfloat16 [1024, 2048], P('seq', 'head'), may hold values from -12 to 12
- values: bfloat16 [1024, 2048], P('seq', 'head'), may hold values from -6 to 6
- block_order: int32 [16], replicated, may hold values from 0 to 15, each once
Outputs:
- attn: bfloat16 [1024, 4096], P(('seq', 'head'))
- lse: float32 [16, 1024], P('head', 'seq')
The draws below stay inside these ranges and needn't reach their ends.
Inputs may be any that keep to these rules, and one draw needn't show every extreme that they name: device-order block j (rows j * 64 to j * 64 + 63) holds sequence positions block_order[j] * 64 onward, in order.
All inputs are finite; a program needn't handle non-finite values.
Results may differ from the reference program's by a relative error of at most 0.006.
Values may be sent and summed in bfloat16 or wider, within the bound.
A program may use at most 128 MiB of HBM per device.

```python
import jax
import jax.numpy as jnp
from jax import lax

HQ = 16
KEY_VALUE_HEADS = 8
HEAD_SIZE = 256
S_DEV = 128
QUERY_GROUP = 2
BLK = 64
NB = 16
SEQUENCE_TOKENS = 1024
N_SEQ = 8


def draw_queries(key, part):
    base_offset = jax.random.truncated_normal(jax.random.fold_in(key, 1), -3.0, 3.0, (SEQUENCE_TOKENS, HQ * HEAD_SIZE), jnp.float32)
    return base_offset.astype(jnp.bfloat16)


def draw_keys(key, part):
    base_offset = jax.random.truncated_normal(jax.random.fold_in(key, 2), -3.0, 3.0, (SEQUENCE_TOKENS, KEY_VALUE_HEADS * HEAD_SIZE), jnp.float32)
    return base_offset.astype(jnp.bfloat16)


def level_of(stream_key, extent, shards, smallest, top_value):
    def one(axis_at, blocks):
        heights = jax.random.uniform(jax.random.fold_in(jax.random.fold_in(stream_key, 6), axis_at), (blocks,), jnp.float32, smallest / len(shards), top_value / len(shards))
        return jnp.repeat(jnp.exp(heights), extent[axis_at] // blocks).reshape((-1,) + (1,) * (len(extent) - axis_at - 1))

    factor_of = one(*shards[0])
    for cut in shards[1:]:
        factor_of = factor_of * one(*cut)
    return factor_of


def scatter_about(key, shape, spread, most, pieces=(), held_as=jnp.bfloat16):
    array = jax.random.normal(key, shape, jnp.float32) * spread
    if len(pieces) > 0:
        array = level_of(key, shape, pieces, -0.22, 0.18) * array
    return jnp.clip(array, min=-most, max=most).astype(held_as)


def setup_inputs(seed: int = 0) -> dict:
    key_of = jax.random.split(jax.random.key(seed), 5)
    queries = draw_queries(jax.random.fold_in(key_of[4], 71), 0)
    keys = draw_keys(jax.random.fold_in(key_of[4], 71), 0)
    values = scatter_about(key_of[2], (SEQUENCE_TOKENS, KEY_VALUE_HEADS * HEAD_SIZE), 1.0, 6.0, ((0, 8), (1, 4)))
    block_order = jax.random.permutation(key_of[3], NB).astype(jnp.int32)
    return {"queries": queries, "keys": keys, "values": values, "block_order": block_order}


def reference(queries, keys, values, block_order):
    rows = jnp.arange(SEQUENCE_TOKENS, dtype=jnp.int32)
    pos = (block_order[rows // BLK] * BLK + rows % BLK).astype(jnp.int32)
    query_head_count = queries.reshape(SEQUENCE_TOKENS, KEY_VALUE_HEADS, QUERY_GROUP, HEAD_SIZE)
    key_single = keys.reshape(SEQUENCE_TOKENS, KEY_VALUE_HEADS, HEAD_SIZE).astype(jnp.float32)
    value_single = values.reshape(SEQUENCE_TOKENS, KEY_VALUE_HEADS, HEAD_SIZE).astype(jnp.float32)
    scale = HEAD_SIZE ** -0.5

    def one_block(index):
        start = (index * S_DEV).astype(jnp.int32)
        query_block = lax.dynamic_slice_in_dim(query_head_count, start, S_DEV, 0).astype(jnp.float32)
        query_pos = lax.dynamic_slice_in_dim(pos, start, S_DEV, 0)
        scores = jnp.einsum('qhgd,khd->hgqk', query_block, key_single) * scale
        allowed = pos[None, :] <= query_pos[:, None]
        scores = jnp.where(allowed, scores, -1e30)
        row_max = jnp.max(scores, axis=-1)
        weights = jnp.where(allowed, jnp.exp(scores - row_max[..., None]), 0.0)
        total = jnp.sum(weights, axis=-1)
        rounded = lax.optimization_barrier(weights.astype(jnp.bfloat16))
        summed = jnp.einsum('hgqk,khd->qhgd', rounded.astype(jnp.float32), value_single)
        output = summed / jnp.transpose(total, (2, 0, 1))[..., None]
        return output.reshape(S_DEV, HQ * HEAD_SIZE).astype(jnp.bfloat16), (row_max + jnp.log(total)).reshape(HQ, S_DEV)

    outputs, sums = lax.map(one_block, jnp.arange(N_SEQ, dtype=jnp.int32))
    attn = outputs.reshape(SEQUENCE_TOKENS, HQ * HEAD_SIZE)
    lse = jnp.transpose(sums, (1, 0, 2)).reshape(HQ, SEQUENCE_TOKENS)
    return attn, lse
```

```python
import functools

import jax
import jax.numpy as jnp
from jax import lax
from jax.experimental import pallas as pl
from jax.experimental.pallas import tpu as pltpu
from jax.sharding import PartitionSpec as P

HEAD_SIZE = 256
QUERY_GROUP = 2
MASKED = -1e30
FLOOR = -1e20
PARTS = 2
MESH = pl.DeviceIdType.MESH


def loop(first, last, body):
    if last - first <= 8:
        for i in range(first, last):
            body(i)
    else:
        lax.fori_loop(first, last, lambda i, c: (body(i), c)[1], 0)


def kernel(
    n, nh, order_hbm, q_hbm, k_hbm, v_hbm, attn, lse,
    qbuf, qout, kvown, kvbuf, maxima, sums, accum, obuf, lse_tx, lse_rx, order,
    load_sem, z_send, y_send, kv_recv, q_sem, o_send, o_recv, l_sem,
):
    head_dim, group = HEAD_SIZE, QUERY_GROUP
    rows = k_hbm.shape[0]
    keep = rows // nh
    part = rows // PARTS
    line = n // 2
    scale = head_dim ** (-0.5)
    me, h = lax.axis_index("seq"), lax.axis_index("head")
    p, y = me // 2, lax.rem(me, 2)
    mine = lax.rem(p, 2)
    mate_p = p + 1 - 2 * mine
    mate = mate_p * 2 + y
    across = p * 2 + 1 - y
    width = group * head_dim

    core = lax.rem(h, 2)

    def far(k):
        q, bit = 0, 1
        while bit < line:
            b, c = lax.rem(p // bit, 2), (k // bit) % 2
            q = q + bit * (b + c - 2 * b * c)
            bit *= 2
        return q

    def turn(i):
        i = jnp.int32(i)
        second = jnp.where(i == 1, line - 1, jnp.where(i == 2, 1, line - i + 1))
        return jnp.where(core == 0, second, i)

    def lanes(start, size):
        return pl.ds(pl.multiple_of(start, head_dim), size)

    loads = []

    def load(src, dst):
        c = pltpu.make_async_copy(src, dst, load_sem.at[len(loads)])
        c.start()
        loads.append(c)

    for i, src in enumerate((k_hbm, v_hbm)):
        for t in range(PARTS):
            load(src.at[pl.ds(t * part, part), lanes(mine * head_dim, head_dim)],
                 kvbuf.at[me, t, i])
    for j in range(2):
        for i, src in enumerate((k_hbm, v_hbm)):
            for t in range(PARTS):
                load(src.at[pl.ds(t * part, part), lanes(j * head_dim, head_dim)],
                     kvown.at[j, t, i])
    for g in range(group):
        load(q_hbm.at[:, lanes(((1 - mine) * group + g) * head_dim, head_dim)],
             qout.at[pl.ds(g * rows, rows)])
    for g in range(group):
        load(q_hbm.at[:, lanes((mine * group + g) * head_dim, head_dim)],
             qbuf.at[0, pl.ds(g * rows, rows)])

    load(order_hbm, order)

    barrier = pltpu.get_barrier_semaphore()

    def greet(s, hh):
        pl.semaphore_signal(barrier, inc=1, device_id=(s, hh), device_id_type=MESH)

    greet(across, h)
    loop(1, line, lambda k: greet(far(k) * 2 + y, h))
    for j in range(1, nh):
        greet(me, lax.rem(h + j, nh))
        greet(mate, lax.rem(h + j, nh))

    maxima[...] = jnp.full_like(maxima, FLOOR)
    sums[...] = jnp.zeros_like(sums)
    accum[...] = jnp.zeros_like(accum)

    pl.semaphore_wait(barrier, 1 + (line - 1) + 2 * (nh - 1))

    def y_copy(q, t):
        slot = q * 2 + y
        return pltpu.make_async_remote_copy(
            src_ref=kvbuf.at[slot, t], dst_ref=kvbuf.at[slot, t],
            send_sem=y_send.at[q, t], recv_sem=kv_recv.at[slot, t],
            device_id=(across, h), device_id_type=MESH)

    def z_copy(k, t):
        q = far(k)
        return pltpu.make_async_remote_copy(
            src_ref=kvown.at[lax.rem(q, 2), t], dst_ref=kvbuf.at[me, t],
            send_sem=z_send.at[k, t], recv_sem=kv_recv.at[me, t],
            device_id=(q * 2 + y, h), device_id_type=MESH)

    def landed(slot, t):
        pltpu.make_async_remote_copy(
            src_ref=kvbuf.at[slot, t], dst_ref=kvbuf.at[slot, t],
            send_sem=y_send.at[0, t], recv_sem=kv_recv.at[slot, t],
            device_id=(across, h), device_id_type=MESH).wait_recv()

    def arrived(slot):
        for t in range(PARTS):
            landed(slot, t)

    q_copy = pltpu.make_async_remote_copy(
        src_ref=qout, dst_ref=qbuf.at[1], send_sem=q_sem.at[0], recv_sem=q_sem.at[1],
        device_id=(mate, h), device_id_type=MESH)

    for c in loads[:2 * PARTS]:
        c.wait()
    for t in range(PARTS):
        y_copy(p, t).start()
    for c in loads[2 * PARTS:]:
        c.wait()

    def send(i):
        for t in range(PARTS):
            z_copy(turn(i), t).start()

    send(1)

    @pl.when(core == 1)
    def _():
        q_copy.start()

    loop(2, line, send)

    @pl.when(core == 0)
    def _():
        q_copy.start()

    row = lax.broadcasted_iota(jnp.int32, (rows, rows), 0)
    col = lax.broadcasted_iota(jnp.int32, (rows, rows), 1)
    per = order.shape[0] // n
    blk = rows // per

    def placed(index, s):
        out = index + order[s * per] * blk
        for b in range(1, per):
            out = jnp.where(index >= b * blk, index + (order[s * per + b] - b) * blk, out)
        return out

    query_pos = [placed(row, s) for s in (me, mate)]

    def attend(rs, slot):
        keys, values = kvbuf[slot, :, 0], kvbuf[slot, :, 1]
        keys, values = (z.reshape(rows, head_dim) for z in (keys, values))
        scores = lax.dot_general(
            qbuf[rs], keys, (((1,), (1,)), ((), ())), preferred_element_type=jnp.float32) * scale
        allowed = placed(col, slot) <= query_pos[rs]
        scores = jnp.where(jnp.concatenate([allowed] * group, 0), scores, MASKED)
        before = maxima[rs]
        fresh = jnp.maximum(before, jnp.max(scores, axis=1, keepdims=True))
        weights = jnp.exp(scores - fresh)
        factor = jnp.exp(before - fresh)
        maxima[rs] = fresh
        sums[rs] = sums[rs] * factor + weights
        update = lax.dot_general(
            weights.astype(jnp.bfloat16), values, (((1,), (0,)), ((), ())),
            preferred_element_type=jnp.float32)
        accum[rs] = accum[rs] * jnp.concatenate([factor] * (head_dim // rows), 1) + update

    attend(0, me)
    arrived(across)
    attend(0, across)

    def step(i):
        q = far(turn(i))
        slot = q * 2 + y
        for t in range(PARTS):
            landed(slot, t)
            y_copy(q, t).start()
        attend(0, slot)

    def step_with_last(i):
        step(i)
        last = far(turn(i - 1)) * 2 + 1 - y
        arrived(last)
        attend(0, last)

    step(1)
    loop(2, line, step_with_last)
    q_copy.wait_recv()
    attend(1, me)
    attend(1, across)

    def catch_up(i):
        q = far(turn(i))
        attend(1, q * 2 + y)
        attend(1, q * 2 + 1 - y)

    loop(1, line - 1, catch_up)
    end = far(turn(line - 1))
    attend(1, end * 2 + y)
    final = end * 2 + 1 - y
    arrived(final)

    def finish(rs):
        attend(rs, final)
        total = jnp.sum(sums[rs], axis=1, keepdims=True)
        out = (accum[rs] / total).astype(jnp.bfloat16)
        for g in range(group):
            obuf[rs, :, g * head_dim:(g + 1) * head_dim] = out[g * rows:(g + 1) * rows]
        return jnp.log(total) + maxima[rs]

    def put_lse(rs, full):
        for g in range(group):
            lse_tx[rs, g:g + 1, :] = jnp.transpose(full[g * rows:(g + 1) * rows])[:1]

    columns = lanes((h * 2 + mine) * width, width)

    def o_copy(rs, j):
        to = lax.rem(h + j, nh)
        return pltpu.make_async_remote_copy(
            src_ref=obuf.at[rs, pl.ds(pl.multiple_of(to * keep, keep), keep)],
            dst_ref=attn.at[:, columns],
            send_sem=o_send.at[rs, j], recv_sem=o_recv.at[rs, h],
            device_id=((me, mate)[rs], to), device_id_type=MESH)

    outs = []
    full = finish(1)
    for j in range(nh):
        outs.append(o_copy(1, j))
        outs[-1].start()
    put_lse(1, full)
    lse_copy = pltpu.make_async_remote_copy(
        src_ref=lse_tx.at[1], dst_ref=lse_rx, send_sem=l_sem.at[0], recv_sem=l_sem.at[1],
        device_id=(mate, h), device_id_type=MESH)
    lse_copy.start()
    full = finish(0)
    for j in range(1, nh):
        outs.append(o_copy(0, j))
        outs[-1].start()
    kept = pltpu.make_async_copy(
        obuf.at[0, pl.ds(pl.multiple_of(h * keep, keep), keep)], attn.at[:, columns],
        o_send.at[0, 0])
    kept.start()
    put_lse(0, full)

    lse_copy.wait_recv()
    own, other = lse_tx[0, :group], lse_rx[:group]
    low = jnp.where(mine == 0, own, other)
    high = jnp.where(mine == 0, other, own)
    lse[...] = jnp.concatenate([low, high], 0)

    for rs in range(2):
        for j in range(1 - rs, nh):
            source = lax.rem(h + j, nh)
            spot = lanes((source * 2 + (mine, 1 - mine)[rs]) * width, width)
            pltpu.make_async_remote_copy(
                src_ref=obuf.at[rs, pl.ds(0, keep)], dst_ref=attn.at[:, spot],
                send_sem=o_send.at[rs, j], recv_sem=o_recv.at[rs, source],
                device_id=(mate, h), device_id_type=MESH).wait_recv()
    kept.wait()
    for c in outs:
        c.wait_send()
    lse_copy.wait_send()
    q_copy.wait_send()
    for t in range(PARTS):
        y_copy(p, t).wait_send()
        loop(1, line, lambda k: (z_copy(k, t).wait_send(), y_copy(far(k), t).wait_send()))


def hand_over(attn, lse, attn_hbm, lse_hbm, sem):
    copies = [
        pltpu.make_async_copy(attn, attn_hbm, sem.at[0]),
        pltpu.make_async_copy(lse, lse_hbm, sem.at[1]),
    ]
    for c in copies:
        c.start()
    for c in copies:
        c.wait()


def local(n, nh, queries, keys, values, block_order):
    rows = queries.shape[0]
    head_dim, group = HEAD_SIZE, QUERY_GROUP
    line = n // 2
    high = group * rows
    bf16, f32 = jnp.bfloat16, jnp.float32
    dma = pltpu.SemaphoreType.DMA
    attn, lse = pl.pallas_call(
        functools.partial(kernel, n, nh),
        out_shape=(
            pltpu.VMEM((rows // nh, queries.shape[1] * nh), bf16),
            pltpu.VMEM((2 * group, rows), f32),
        ),
        in_specs=[pl.BlockSpec(memory_space=pl.ANY)] * 4,
        out_specs=(pl.BlockSpec(memory_space=pltpu.VMEM),) * 2,
        scratch_shapes=[
            pltpu.VMEM((2, high, head_dim), bf16),
            pltpu.VMEM((high, head_dim), bf16),
            pltpu.VMEM((2, PARTS, 2, rows // PARTS, head_dim), bf16),
            pltpu.VMEM((n, PARTS, 2, rows // PARTS, head_dim), bf16),
            pltpu.VMEM((2, high, rows), f32),
            pltpu.VMEM((2, high, rows), f32),
            pltpu.VMEM((2, high, head_dim), f32),
            pltpu.VMEM((2, rows, group * head_dim), bf16),
            pltpu.VMEM((2, 8, rows), f32),
            pltpu.VMEM((8, rows), f32),
            pltpu.SMEM(block_order.shape, jnp.int32),
            dma((6 * PARTS + 2 * group + 1,)),
            dma((line, PARTS)),
            dma((line, PARTS)),
            dma((n, PARTS)),
            dma((2,)),
            dma((2, nh)),
            dma((2, nh)),
            dma((2,)),
        ],
        compiler_params=pltpu.CompilerParams(collective_id=0, has_side_effects=True),
    )(block_order, queries, keys, values)
    attn, lse = (pltpu.with_memory_space_constraint(z, pltpu.VMEM) for z in (attn, lse))
    return pl.pallas_call(
        hand_over,
        out_shape=(pltpu.HBM(attn.shape, bf16), pltpu.HBM(lse.shape, f32)),
        in_specs=[pl.BlockSpec(memory_space=pltpu.VMEM)] * 2,
        out_specs=(pl.BlockSpec(memory_space=pltpu.HBM),) * 2,
        scratch_shapes=[dma((2,))],
    )(attn, lse)


def solution(mesh):
    in_specs = (P("seq", "head"), P("seq", "head"), P("seq", "head"), P())
    out_specs = (P(("seq", "head"), None), P("head", "seq"))
    body = functools.partial(local, mesh.shape["seq"], mesh.shape["head"])
    return jax.shard_map(body, mesh=mesh, in_specs=in_specs, out_specs=out_specs, check_vma=False)
```

```python
import functools

import jax
import jax.numpy as jnp
from jax import lax
from jax.experimental import pallas as pl
from jax.experimental.pallas import tpu as pltpu
from jax.sharding import PartitionSpec as P

HEAD_SIZE = 256
QUERY_GROUP = 2
MASKED = -1e30
FLOOR = -1e20
PARTS = 1
TEAM = 4
MESH = pl.DeviceIdType.MESH


def loop(first, last, body):
    if last - first <= 8:
        for i in range(first, last):
            body(i)
    else:
        lax.fori_loop(first, last, lambda i, c: (body(i), c)[1], 0)


def kernel(
    n, nh, order_hbm, q_hbm, k_hbm, v_hbm, attn, lse,
    qbuf, qout, kvout, kvbuf, maxima, sums, accum, obuf, lse_tx, lse_rx, order,
    load_sem, cross_sem, near_sem, share_sem, kv_recv, q_send, q_recv,
    o_send, o_recv, l_send, l_recv, ready, plane_ready,
):
    head_dim, group = HEAD_SIZE, QUERY_GROUP
    rows = k_hbm.shape[0]
    keep = rows // nh
    part = rows // PARTS
    teams, planes = n // TEAM, nh // 2
    scale = head_dim ** (-0.5)
    width = group * head_dim
    me, h = lax.axis_index("seq"), lax.axis_index("head")
    x, c = h // 2, lax.rem(h, 2)
    g, j = me // TEAM, lax.rem(me, TEAM)
    y = lax.rem(j, 2)
    keeper = 1 - j // 2
    own = c == keeper
    other = jnp.logical_not(own)
    base = 2 * (1 - c)
    partner = x * 2 + 1 - c
    upper = j // 2

    def rank(m):
        return m // 2 + 2 * (m % 2)

    place = upper + 2 * y


    def lanes(start, size):
        return pl.ds(pl.multiple_of(start, head_dim), size)

    barrier = pltpu.get_barrier_semaphore()

    def signal(sem, s, hh):
        pl.semaphore_signal(sem, inc=1, device_id=(s, hh), device_id_type=MESH)

    for m in range(TEAM):
        @pl.when(rank(m) > place)
        def _():
            signal(barrier, g * TEAM + m, x * 2)
            signal(barrier, g * TEAM + m, x * 2 + 1)

    def greet_team(d):
        @pl.when(g + d < teams)
        def _():
            for i in range(2):
                signal(barrier, (g + d) * TEAM + base + i, x * 2 + 1)

            @pl.when(c == 1)
            def _():
                for m in range(TEAM):
                    signal(barrier, (g + d) * TEAM + m, x * 2 + keeper)

    loop(1, teams, greet_team)

    @pl.when(c == 0)
    def _():
        signal(barrier, me, partner)

    for xx in range(planes):
        @pl.when(xx > x)
        def _():
            signal(barrier, me, xx * 2 + c)

    def load(src, dst, i):
        pltpu.make_async_copy(src, dst, load_sem.at[i]).start()

    for i in range(2):
        for g2 in range(group):
            load(q_hbm.at[:, lanes((i * group + g2) * head_dim, head_dim)],
                 qout.at[i, pl.ds(g2 * rows, rows)], 0)
    for i in range(2):
        for t in range(PARTS):
            for z, src in enumerate((k_hbm, v_hbm)):
                load(src.at[pl.ds(t * part, part), lanes(i * head_dim, head_dim)],
                     kvout.at[i, t, z], 0)

    @pl.when(own)
    def _():
        for g2 in range(group):
            load(q_hbm.at[:, lanes((y * group + g2) * head_dim, head_dim)],
                 qbuf.at[y, pl.ds(g2 * rows, rows)], 1)
        for t in range(PARTS):
            for z, src in enumerate((k_hbm, v_hbm)):
                load(src.at[pl.ds(t * part, part), lanes(y * head_dim, head_dim)],
                     kvbuf.at[me, t, z], 1)

    order_copy = pltpu.make_async_copy(order_hbm, order, load_sem.at[2])
    order_copy.start()

    def wait(sem, count):
        @pl.when(count > 0)
        def _():
            pl.semaphore_wait(sem, count)

    wait(barrier, 2 * place + c + x + g * (2 + 4 * c))

    for m in range(TEAM):
        @pl.when(rank(m) < place)
        def _():
            signal(ready.at[me], g * TEAM + m, x * 2)
            signal(ready.at[me], g * TEAM + m, x * 2 + 1)

    @pl.when(c == 1)
    def _():
        signal(ready.at[me], me, partner)

        def answer_team(d):
            @pl.when(g - d >= 0)
            def _():
                for m in range(TEAM):
                    signal(ready.at[me], (g - d) * TEAM + m, x * 2 + keeper)

        loop(1, teams, answer_team)

    def q_copy(i):
        return pltpu.make_async_remote_copy(
            src_ref=qout.at[i], dst_ref=qbuf.at[y], send_sem=q_send, recv_sem=q_recv.at[y],
            device_id=(g * TEAM + base + i, x * 2 + keeper), device_id_type=MESH)

    def kv_copy(i, t, team, core, sem):
        return pltpu.make_async_remote_copy(
            src_ref=kvout.at[i, t], dst_ref=kvbuf.at[me, t],
            send_sem=sem, recv_sem=kv_recv.at[me, t],
            device_id=(team * TEAM + base + i, x * 2 + core), device_id_type=MESH)

    def share(slot, t):
        return pltpu.make_async_remote_copy(
            src_ref=kvbuf.at[slot, t], dst_ref=kvbuf.at[slot, t],
            send_sem=share_sem, recv_sem=kv_recv.at[slot, t],
            device_id=(me, partner), device_id_type=MESH)

    def ask(i):
        q_copy(i).start()

    def near(i):
        for t in range(PARTS):
            kv_copy(i, t, g, 0, near_sem).start()

    def cross(team):
        for i in range(2):
            for t in range(PARTS):
                kv_copy(i, t, team, 1, cross_sem).start()

    for i, whole in ((0, (qout, kvout)), ):
        for z in whole:
            pltpu.make_async_copy(z, z, load_sem.at[i]).wait()

    pair = [y, 1 - y]
    spot = [(1 - c) + 2 * i for i in pair]

    def cross_back(d):
        @pl.when(g - d >= 0)
        def _():
            cross(g - d)

    def cross_on(d):
        @pl.when(g + d < teams)
        def _():
            for i in range(2):
                pl.semaphore_wait(ready.at[(g + d) * TEAM + base + i], 1)
            cross(g + d)

    for i, r in zip(pair, spot):
        pl.when(r < place)(functools.partial(ask, i))
    loop(1, teams, cross_back)
    for i, r in zip(pair, spot):
        pl.when(r < place)(functools.partial(near, i))

    for i, r in zip(pair, spot):
        @pl.when(r > place)
        def _():
            pl.semaphore_wait(ready.at[g * TEAM + base + i], 2)
            ask(i)

    for i, r in zip(pair, spot):
        pl.when(r > place)(functools.partial(near, i))

    @pl.when(c == 0)
    def _():
        pl.semaphore_wait(ready.at[me], 1)

    @pl.when(own)
    def _():
        for z in (qbuf.at[0], kvbuf.at[0]):
            pltpu.make_async_copy(z, z, load_sem.at[1]).wait()
        for t in range(PARTS):
            share(me, t).start()

    loop(1, teams, cross_on)

    maxima[...] = jnp.full_like(maxima, FLOOR)
    sums[...] = jnp.zeros_like(sums)
    accum[...] = jnp.zeros_like(accum)
    order_copy.wait()

    row = lax.broadcasted_iota(jnp.int32, (rows, rows), 0)
    col = lax.broadcasted_iota(jnp.int32, (rows, rows), 1)
    per = order.shape[0] // n
    blk = rows // per

    def placed(index, s):
        out = index + order[s * per] * blk
        for b in range(1, per):
            out = jnp.where(index >= b * blk, index + (order[s * per + b] - b) * blk, out)
        return out

    query_pos = [placed(row, g * TEAM + base + rs) for rs in range(2)]

    def fold(z):
        return z.reshape(rows, head_dim)

    def attend(parts, slots):
        for rs in parts:
            scores = []
            for slot in slots:
                one = lax.dot_general(
                    qbuf[rs], fold(kvbuf[slot, :, 0]), (((1,), (1,)), ((), ())),
                    preferred_element_type=jnp.float32) * scale
                allowed = placed(col, slot) <= query_pos[rs]
                scores.append(jnp.where(jnp.concatenate([allowed] * group, 0), one, MASKED))
            before = maxima[rs]
            top = functools.reduce(jnp.maximum, scores)
            fresh = jnp.maximum(before, jnp.max(top, axis=1, keepdims=True))
            factor = jnp.exp(before - fresh)
            maxima[rs] = fresh
            weights = [jnp.exp(one - fresh) for one in scores]
            sums[rs] = sums[rs] * factor + functools.reduce(jnp.add, weights)
            update = [
                lax.dot_general(
                    w.astype(jnp.bfloat16), fold(kvbuf[slot, :, 1]), (((1,), (0,)), ((), ())),
                    preferred_element_type=jnp.float32)
                for w, slot in zip(weights, slots)]
            accum[rs] = accum[rs] * jnp.concatenate(
                [factor] * (head_dim // rows), 1) + functools.reduce(jnp.add, update)

    def landed(slot, t):
        share(slot, t).wait_recv()

    def take(slot, core):
        for t in range(PARTS):
            landed(slot, t)

            @pl.when(c == core)
            def _():
                share(slot, t).start()
        return slot

    @pl.when(other)
    def _():
        for t in range(PARTS):
            landed(me, t)

    for rs in range(2):
        @pl.when(other | (y != rs))
        def _():
            pltpu.make_async_remote_copy(
                src_ref=qout.at[0], dst_ref=qbuf.at[rs], send_sem=q_send,
                recv_sem=q_recv.at[rs], device_id=(me, partner), device_id_type=MESH).wait_recv()

    attend((0, 1), (me,))

    beside = g * TEAM + j + 1 - 2 * y
    above = g * TEAM + lax.rem(j + 2, TEAM)
    across = above + 1 - 2 * y
    for m in range(TEAM):
        @pl.when((m // 2 == c) & (rank(m) > place))
        def _():
            pl.semaphore_wait(ready.at[g * TEAM + m], 2)

    for xx in range(planes):
        @pl.when(xx < x)
        def _():
            signal(plane_ready, me, xx * 2 + c)

    wait(plane_ready, planes - 1 - x)

    for xx in range(planes):
        @pl.when(xx > x)
        def _():
            signal(plane_ready, me, xx * 2 + c)

    def wait_for(slot):
        for t in range(PARTS):
            landed(slot, t)
        return slot

    def pass_on(slot):
        for t in range(PARTS):
            landed(slot, t)
            share(slot, t).start()
        return slot

    both = (0, 1)
    if teams == 2:
        there = (1 - g) * TEAM
        lead = jnp.where(y == 0, 2 * g, 2 - 2 * g)
        far = [there + lead, there + lead + 1, there + 2 - lead, there + 3 - lead]


        @pl.when(c == 0)
        def _():
            attend(both, (pass_on(beside),))
            attend(both, [wait_for(s) for s in far[:2]])

        @pl.when(c == 1)
        def _():
            for s in far[:2]:
                pass_on(s)
            attend(both, (wait_for(beside),))
            attend(both, far[:2])

        first = (g == 0) | (c == 0)
        way = jnp.where(first, 0, 1)
        close = (above, across)
        now = [jnp.where(first, a, b) for a, b in zip(close, far[2:])]
        final = [jnp.where(first, b, a) for a, b in zip(close, far[2:])]
        attend(both, [take(s, way) for s in now])
        for s in final:
            take(s, 1 - way)
    else:
        attend(both, [take(s, 0) for s in (beside, above, across)])

        def slot_of(k):
            return lax.rem(g + 1 + k // TEAM, teams) * TEAM + lax.rem(k, TEAM)

        def further(k):
            attend(both, (take(slot_of(jnp.int32(k)), 1),))

        loop(0, TEAM * (teams - 1) - 1, further)
        final = [slot_of(jnp.int32(TEAM * (teams - 1) - 1))]
        take(final[0], 1)

    def finish(rs):
        attend((rs,), final)
        total = jnp.sum(sums[rs], axis=1, keepdims=True)
        out = (accum[rs] / total).astype(jnp.bfloat16)
        for g2 in range(group):
            obuf[rs, :, g2 * head_dim:(g2 + 1) * head_dim] = out[g2 * rows:(g2 + 1) * rows]
        return jnp.log(total) + maxima[rs]

    columns = lanes(((x * 2 + keeper) * 2 + y) * width, width)
    wait(plane_ready, x)

    def send_out(rs):
        mine = own & (y == rs)
        for k in range(nh):
            to = lax.rem(x + 1 + k, planes) * 2 + lax.rem(c + 1 + k // planes, 2)
            src = obuf.at[rs, pl.ds(pl.multiple_of(to * keep, keep), keep)]

            def away():
                pltpu.make_async_remote_copy(
                    src_ref=src, dst_ref=attn.at[:, columns], send_sem=o_send, recv_sem=o_recv,
                    device_id=(g * TEAM + base + rs, to), device_id_type=MESH).start()

            if k < nh - 1:
                away()
            else:
                pl.when(jnp.logical_not(mine))(away)

                @pl.when(mine)
                def _():
                    pltpu.make_async_copy(src, attn.at[:, columns], o_send).start()

    def send_lse(rs, full):
        for g2 in range(group):
            lse_tx[rs, g2:g2 + 1, :] = jnp.transpose(full[g2 * rows:(g2 + 1) * rows])[:1]
        mine = own & (y == rs)

        @pl.when(jnp.logical_not(mine))
        def _():
            pltpu.make_async_remote_copy(
                src_ref=lse_tx.at[rs], dst_ref=lse_rx.at[y], send_sem=l_send, recv_sem=l_recv,
                device_id=(g * TEAM + base + rs, x * 2 + keeper), device_id_type=MESH).start()

        @pl.when(mine)
        def _():
            lse_rx[rs] = lse_tx[rs]

    fulls = []
    for rs in range(2):
        fulls.append(finish(rs))
        send_out(rs)
    for rs in range(2):
        send_lse(rs, fulls[rs])

    def drain(ref, sem):
        pltpu.make_async_copy(ref, ref, sem).wait()

    def by_kind(ref, less, sem):
        pl.when(own)(lambda: drain(less, sem))
        pl.when(other)(lambda: drain(ref, sem))

    by_kind(lse_rx, lse_rx.at[pl.ds(0, 1)], l_recv)
    lse[...] = jnp.concatenate([lse_rx[0, :group], lse_rx[1, :group]], 0)
    by_kind(attn, attn.at[:, pl.ds(0, (2 * nh - 1) * width)], o_recv)
    drain(attn, o_send)
    by_kind(lse_tx, lse_tx.at[pl.ds(0, 1)], l_send)
    by_kind(qbuf, qbuf.at[pl.ds(0, 1)], q_send)
    by_kind(kvbuf.at[pl.ds(0, 2)], kvbuf.at[pl.ds(0, 1)], near_sem)
    drain(kvbuf.at[pl.ds(0, 2 * (teams - 1))], cross_sem)
    for core, count in ((0, TEAM - 1), (1, TEAM * (teams - 1))):
        pl.when((c == core) & own)(
            functools.partial(drain, kvbuf.at[pl.ds(0, count + 1)], share_sem))
        pl.when((c == core) & other)(
            functools.partial(drain, kvbuf.at[pl.ds(0, count)], share_sem))


def hand_over(attn, lse, attn_hbm, lse_hbm, sem):
    copies = [
        pltpu.make_async_copy(attn, attn_hbm, sem.at[0]),
        pltpu.make_async_copy(lse, lse_hbm, sem.at[1]),
    ]
    for c in copies:
        c.start()
    for c in copies:
        c.wait()


def local(n, nh, queries, keys, values, block_order):
    rows = queries.shape[0]
    head_dim, group = HEAD_SIZE, QUERY_GROUP
    high = group * rows
    bf16, f32 = jnp.bfloat16, jnp.float32
    dma = pltpu.SemaphoreType.DMA
    attn, lse = pl.pallas_call(
        functools.partial(kernel, n, nh),
        out_shape=(
            pltpu.VMEM((rows // nh, queries.shape[1] * nh), bf16),
            pltpu.VMEM((2 * group, rows), f32),
        ),
        in_specs=[pl.BlockSpec(memory_space=pl.ANY)] * 4,
        out_specs=(pl.BlockSpec(memory_space=pltpu.VMEM),) * 2,
        scratch_shapes=[
            pltpu.VMEM((2, high, head_dim), bf16),
            pltpu.VMEM((2, high, head_dim), bf16),
            pltpu.VMEM((2, PARTS, 2, rows // PARTS, head_dim), bf16),
            pltpu.VMEM((n, PARTS, 2, rows // PARTS, head_dim), bf16),
            pltpu.VMEM((2, high, rows), f32),
            pltpu.VMEM((2, high, rows), f32),
            pltpu.VMEM((2, high, head_dim), f32),
            pltpu.VMEM((2, rows, group * head_dim), bf16),
            pltpu.VMEM((2, 8, rows), f32),
            pltpu.VMEM((2, 8, rows), f32),
            pltpu.SMEM(block_order.shape, jnp.int32),
            dma((3,)),
            dma,
            dma,
            dma,
            dma((n, PARTS)),
            dma,
            dma((2,)),
            dma,
            dma,
            dma,
            dma,
            pltpu.SemaphoreType.REGULAR((n,)),
            pltpu.SemaphoreType.REGULAR,
        ],
        compiler_params=pltpu.CompilerParams(collective_id=0, has_side_effects=True),
    )(block_order, queries, keys, values)
    attn, lse = (pltpu.with_memory_space_constraint(z, pltpu.VMEM) for z in (attn, lse))
    return pl.pallas_call(
        hand_over,
        out_shape=(pltpu.HBM(attn.shape, bf16), pltpu.HBM(lse.shape, f32)),
        in_specs=[pl.BlockSpec(memory_space=pltpu.VMEM)] * 2,
        out_specs=(pl.BlockSpec(memory_space=pltpu.HBM),) * 2,
        scratch_shapes=[dma((2,))],
    )(attn, lse)


def solution(mesh):
    in_specs = (P("seq", "head"), P("seq", "head"), P("seq", "head"), P())
    out_specs = (P(("seq", "head"), None), P("head", "seq"))
    body = functools.partial(local, mesh.shape["seq"], mesh.shape["head"])
    return jax.shard_map(body, mesh=mesh, in_specs=in_specs, out_specs=out_specs, check_vma=False)
```

```python
import functools

import jax
import jax.numpy as jnp
from jax import lax
from jax.experimental import pallas as pl
from jax.experimental.pallas import tpu as pltpu
from jax.sharding import PartitionSpec as P

HEAD_SIZE = 256
QUERY_GROUP = 2
MASKED = -1e30
FLOOR = -1e20
PARTS = 1
TEAM = 4
MESH = pl.DeviceIdType.MESH


def loop(first, last, body):
    if last - first <= 8:
        for i in range(first, last):
            body(i)
    else:
        lax.fori_loop(first, last, lambda i, c: (body(i), c)[1], 0)


def kernel(
    n, nh, order_hbm, q_hbm, k_hbm, v_hbm, attn, lse,
    qbuf, qout, kvout, kvbuf, maxima, sums, accum, obuf, lse_tx, lse_rx, order,
    load_sem, cross_sem, near_sem, share_sem, kv_recv, q_send, q_recv,
    o_send, o_recv, l_send, l_recv, ready, plane_ready,
):
    head_dim, group = HEAD_SIZE, QUERY_GROUP
    rows = k_hbm.shape[0]
    keep = rows // nh
    part = rows // PARTS
    teams, planes = n // TEAM, nh // 2
    scale = head_dim ** (-0.5)
    width = group * head_dim
    me, h = lax.axis_index("seq"), lax.axis_index("head")
    x, c = h // 2, lax.rem(h, 2)
    g, j = me // TEAM, lax.rem(me, TEAM)
    y = lax.rem(j, 2)
    keeper = 1 - j // 2
    own = c == keeper
    other = jnp.logical_not(own)
    base = 2 * (1 - c)
    partner = x * 2 + 1 - c
    upper = j // 2

    def rank(m):
        return m // 2 + 2 * (m % 2)

    place = upper + 2 * y


    def lanes(start, size):
        return pl.ds(pl.multiple_of(start, head_dim), size)

    barrier = pltpu.get_barrier_semaphore()

    def signal(sem, s, hh):
        pl.semaphore_signal(sem, inc=1, device_id=(s, hh), device_id_type=MESH)

    for m in range(TEAM):
        @pl.when(rank(m) > place)
        def _():
            signal(barrier, g * TEAM + m, x * 2)
            signal(barrier, g * TEAM + m, x * 2 + 1)

    def greet_team(d):
        @pl.when(g + d < teams)
        def _():
            for i in range(2):
                signal(barrier, (g + d) * TEAM + base + i, x * 2 + 1)

            @pl.when(c == 1)
            def _():
                for m in range(TEAM):
                    signal(barrier, (g + d) * TEAM + m, x * 2 + keeper)

    loop(1, teams, greet_team)

    @pl.when(c == 0)
    def _():
        signal(barrier, me, partner)

    for xx in range(planes):
        @pl.when(xx > x)
        def _():
            signal(barrier, me, xx * 2 + c)

    def load(src, dst, i):
        pltpu.make_async_copy(src, dst, load_sem.at[i]).start()

    for i in range(2):
        for g2 in range(group):
            load(q_hbm.at[:, lanes((i * group + g2) * head_dim, head_dim)],
                 qout.at[i, pl.ds(g2 * rows, rows)], 0)
    for i in range(2):
        for t in range(PARTS):
            for z, src in enumerate((k_hbm, v_hbm)):
                load(src.at[pl.ds(t * part, part), lanes(i * head_dim, head_dim)],
                     kvout.at[i, t, z], 0)

    @pl.when(own)
    def _():
        for g2 in range(group):
            load(q_hbm.at[:, lanes((y * group + g2) * head_dim, head_dim)],
                 qbuf.at[y, pl.ds(g2 * rows, rows)], 1)
        for t in range(PARTS):
            for z, src in enumerate((k_hbm, v_hbm)):
                load(src.at[pl.ds(t * part, part), lanes(y * head_dim, head_dim)],
                     kvbuf.at[me, t, z], 1)

    order_copy = pltpu.make_async_copy(order_hbm, order, load_sem.at[2])
    order_copy.start()

    def wait(sem, count):
        @pl.when(count > 0)
        def _():
            pl.semaphore_wait(sem, count)

    wait(barrier, 2 * place + c + x + g * (2 + 4 * c))

    for m in range(TEAM):
        @pl.when(rank(m) < place)
        def _():
            signal(ready.at[me], g * TEAM + m, x * 2)
            signal(ready.at[me], g * TEAM + m, x * 2 + 1)

    @pl.when(c == 1)
    def _():
        signal(ready.at[me], me, partner)

        def answer_team(d):
            @pl.when(g - d >= 0)
            def _():
                for m in range(TEAM):
                    signal(ready.at[me], (g - d) * TEAM + m, x * 2 + keeper)

        loop(1, teams, answer_team)

    def q_copy(i):
        return pltpu.make_async_remote_copy(
            src_ref=qout.at[i], dst_ref=qbuf.at[y], send_sem=q_send, recv_sem=q_recv.at[y],
            device_id=(g * TEAM + base + i, x * 2 + keeper), device_id_type=MESH)

    def kv_copy(i, t, team, core, sem):
        return pltpu.make_async_remote_copy(
            src_ref=kvout.at[i, t], dst_ref=kvbuf.at[me, t],
            send_sem=sem, recv_sem=kv_recv.at[me, t],
            device_id=(team * TEAM + base + i, x * 2 + core), device_id_type=MESH)

    def share(slot, t):
        return pltpu.make_async_remote_copy(
            src_ref=kvbuf.at[slot, t], dst_ref=kvbuf.at[slot, t],
            send_sem=share_sem, recv_sem=kv_recv.at[slot, t],
            device_id=(me, partner), device_id_type=MESH)

    def ask(i):
        q_copy(i).start()

    def near(i):
        for t in range(PARTS):
            kv_copy(i, t, g, 0, near_sem).start()

    def cross(team):
        for i in range(2):
            for t in range(PARTS):
                kv_copy(i, t, team, 1, cross_sem).start()

    for i, whole in ((0, (qout, kvout)), ):
        for z in whole:
            pltpu.make_async_copy(z, z, load_sem.at[i]).wait()

    pair = [y, 1 - y]
    spot = [(1 - c) + 2 * i for i in pair]

    def cross_back(d):
        @pl.when(g - d >= 0)
        def _():
            cross(g - d)

    def cross_on(d):
        @pl.when(g + d < teams)
        def _():
            for i in range(2):
                pl.semaphore_wait(ready.at[(g + d) * TEAM + base + i], 1)
            cross(g + d)

    def ask_both():
        for i, r in zip(pair, spot):
            @pl.when(r > place)
            def _():
                pl.semaphore_wait(ready.at[g * TEAM + base + i], 2)

            pl.when(r != place)(functools.partial(ask, i))

    pl.when(spot[0] < place)(ask_both)
    loop(1, teams, cross_back)
    pl.when(spot[0] >= place)(ask_both)
    for i, r in zip(pair, spot):
        pl.when(r != place)(functools.partial(near, i))

    @pl.when(c == 0)
    def _():
        pl.semaphore_wait(ready.at[me], 1)

    @pl.when(own)
    def _():
        for z in (qbuf.at[0], kvbuf.at[0]):
            pltpu.make_async_copy(z, z, load_sem.at[1]).wait()
        for t in range(PARTS):
            share(me, t).start()

    loop(1, teams, cross_on)

    maxima[...] = jnp.full_like(maxima, FLOOR)
    sums[...] = jnp.zeros_like(sums)
    accum[...] = jnp.zeros_like(accum)
    order_copy.wait()

    row = lax.broadcasted_iota(jnp.int32, (rows, rows), 0)
    col = lax.broadcasted_iota(jnp.int32, (rows, rows), 1)
    per = order.shape[0] // n
    blk = rows // per

    def placed(index, s):
        out = index + order[s * per] * blk
        for b in range(1, per):
            out = jnp.where(index >= b * blk, index + (order[s * per + b] - b) * blk, out)
        return out

    query_pos = [placed(row, g * TEAM + base + rs) for rs in range(2)]

    def fold(z):
        return z.reshape(rows, head_dim)

    def attend(parts, slots):
        for rs in parts:
            scores = []
            for slot in slots:
                one = lax.dot_general(
                    qbuf[rs], fold(kvbuf[slot, :, 0]), (((1,), (1,)), ((), ())),
                    preferred_element_type=jnp.float32) * scale
                allowed = placed(col, slot) <= query_pos[rs]
                scores.append(jnp.where(jnp.concatenate([allowed] * group, 0), one, MASKED))
            before = maxima[rs]
            top = functools.reduce(jnp.maximum, scores)
            fresh = jnp.maximum(before, jnp.max(top, axis=1, keepdims=True))
            factor = jnp.exp(before - fresh)
            maxima[rs] = fresh
            weights = [jnp.exp(one - fresh) for one in scores]
            sums[rs] = sums[rs] * factor + functools.reduce(jnp.add, weights)
            update = [
                lax.dot_general(
                    w.astype(jnp.bfloat16), fold(kvbuf[slot, :, 1]), (((1,), (0,)), ((), ())),
                    preferred_element_type=jnp.float32)
                for w, slot in zip(weights, slots)]
            accum[rs] = accum[rs] * jnp.concatenate(
                [factor] * (head_dim // rows), 1) + functools.reduce(jnp.add, update)

    def landed(slot, t):
        share(slot, t).wait_recv()

    def take(slot, core):
        for t in range(PARTS):
            landed(slot, t)

            @pl.when(c == core)
            def _():
                share(slot, t).start()
        return slot

    @pl.when(other)
    def _():
        for t in range(PARTS):
            landed(me, t)

    for rs in range(2):
        @pl.when(other | (y != rs))
        def _():
            pltpu.make_async_remote_copy(
                src_ref=qout.at[0], dst_ref=qbuf.at[rs], send_sem=q_send,
                recv_sem=q_recv.at[rs], device_id=(me, partner), device_id_type=MESH).wait_recv()

    attend((0, 1), (me,))

    beside = g * TEAM + j + 1 - 2 * y
    above = g * TEAM + lax.rem(j + 2, TEAM)
    across = above + 1 - 2 * y
    for m in range(TEAM):
        @pl.when((m // 2 == c) & (rank(m) > place))
        def _():
            pl.semaphore_wait(ready.at[g * TEAM + m], 2)

    for xx in range(planes):
        @pl.when(xx < x)
        def _():
            signal(plane_ready, me, xx * 2 + c)

    def wait_for(slot):
        for t in range(PARTS):
            landed(slot, t)
        return slot

    def pass_on(slot):
        for t in range(PARTS):
            landed(slot, t)
            share(slot, t).start()
        return slot

    both = (0, 1)
    if teams == 2:
        there = (1 - g) * TEAM
        close = (above, across)
        lead = jnp.where(y == 0, 2 * g, 2 - 2 * g)
        far = [there + lead, there + lead + 1, there + 2 - lead, there + 3 - lead]


        @pl.when(c == 0)
        def _():
            attend(both, (pass_on(beside),))
            attend(both, [pass_on(s) for s in close])

        @pl.when(c == 1)
        def _():
            for s in far[:2]:
                pass_on(s)
            attend(both, (wait_for(beside),))
            attend(both, far[:2])

        now = [jnp.where(c == 0, a, b) for a, b in zip(far[:2], far[2:])]
        final = [jnp.where(c == 0, a, b) for a, b in zip(far[2:], close)]
        wait(plane_ready, planes - 1 - x)

        for xx in range(planes):
            @pl.when(xx > x)
            def _():
                signal(plane_ready, me, xx * 2 + c)

        attend(both, [take(s, 1) for s in now])
        for s in final:
            wait_for(s)
    else:
        attend(both, [take(s, 0) for s in (beside, above, across)])
        wait(plane_ready, planes - 1 - x)

        for xx in range(planes):
            @pl.when(xx > x)
            def _():
                signal(plane_ready, me, xx * 2 + c)

        def slot_of(k):
            return lax.rem(g + 1 + k // TEAM, teams) * TEAM + lax.rem(k, TEAM)

        def further(k):
            attend(both, (take(slot_of(jnp.int32(k)), 1),))

        loop(0, TEAM * (teams - 1) - 1, further)
        final = [slot_of(jnp.int32(TEAM * (teams - 1) - 1))]
        take(final[0], 1)

    def finish(rs):
        attend((rs,), final)
        total = jnp.sum(sums[rs], axis=1, keepdims=True)
        out = (accum[rs] / total).astype(jnp.bfloat16)
        for g2 in range(group):
            obuf[rs, :, g2 * head_dim:(g2 + 1) * head_dim] = out[g2 * rows:(g2 + 1) * rows]
        return jnp.log(total) + maxima[rs]

    columns = lanes(((x * 2 + keeper) * 2 + y) * width, width)
    wait(plane_ready, x)

    def send_out(rs):
        mine = own & (y == rs)
        for k in range(nh):
            to = lax.rem(x + 1 + k, planes) * 2 + lax.rem(c + 1 + k // planes, 2)
            src = obuf.at[rs, pl.ds(pl.multiple_of(to * keep, keep), keep)]

            def away():
                pltpu.make_async_remote_copy(
                    src_ref=src, dst_ref=attn.at[:, columns], send_sem=o_send, recv_sem=o_recv,
                    device_id=(g * TEAM + base + rs, to), device_id_type=MESH).start()

            if k < nh - 1:
                away()
            else:
                pl.when(jnp.logical_not(mine))(away)

                @pl.when(mine)
                def _():
                    pltpu.make_async_copy(src, attn.at[:, columns], o_send).start()

    def send_lse(rs, full):
        for g2 in range(group):
            lse_tx[rs, g2:g2 + 1, :] = jnp.transpose(full[g2 * rows:(g2 + 1) * rows])[:1]
        mine = own & (y == rs)

        @pl.when(jnp.logical_not(mine))
        def _():
            pltpu.make_async_remote_copy(
                src_ref=lse_tx.at[rs], dst_ref=lse_rx.at[y], send_sem=l_send, recv_sem=l_recv,
                device_id=(g * TEAM + base + rs, x * 2 + keeper), device_id_type=MESH).start()

        @pl.when(mine)
        def _():
            lse_rx[rs] = lse_tx[rs]

    fulls = []
    for rs in range(2):
        fulls.append(finish(rs))
        send_out(rs)
    for rs in range(2):
        send_lse(rs, fulls[rs])

    def drain(ref, sem):
        pltpu.make_async_copy(ref, ref, sem).wait()

    def by_kind(ref, less, sem):
        pl.when(own)(lambda: drain(less, sem))
        pl.when(other)(lambda: drain(ref, sem))

    by_kind(lse_rx, lse_rx.at[pl.ds(0, 1)], l_recv)
    lse[...] = jnp.concatenate([lse_rx[0, :group], lse_rx[1, :group]], 0)
    by_kind(attn, attn.at[:, pl.ds(0, (2 * nh - 1) * width)], o_recv)
    drain(attn, o_send)
    by_kind(lse_tx, lse_tx.at[pl.ds(0, 1)], l_send)
    by_kind(qbuf, qbuf.at[pl.ds(0, 1)], q_send)
    by_kind(kvbuf.at[pl.ds(0, 2)], kvbuf.at[pl.ds(0, 1)], near_sem)
    drain(kvbuf.at[pl.ds(0, 2 * (teams - 1))], cross_sem)
    for core, count in ((0, TEAM - 1), (1, TEAM * (teams - 1))):
        pl.when((c == core) & own)(
            functools.partial(drain, kvbuf.at[pl.ds(0, count + 1)], share_sem))
        pl.when((c == core) & other)(
            functools.partial(drain, kvbuf.at[pl.ds(0, count)], share_sem))


def hand_over(attn, lse, attn_hbm, lse_hbm, sem):
    copies = [
        pltpu.make_async_copy(attn, attn_hbm, sem.at[0]),
        pltpu.make_async_copy(lse, lse_hbm, sem.at[1]),
    ]
    for c in copies:
        c.start()
    for c in copies:
        c.wait()


def local(n, nh, queries, keys, values, block_order):
    rows = queries.shape[0]
    head_dim, group = HEAD_SIZE, QUERY_GROUP
    high = group * rows
    bf16, f32 = jnp.bfloat16, jnp.float32
    dma = pltpu.SemaphoreType.DMA
    attn, lse = pl.pallas_call(
        functools.partial(kernel, n, nh),
        out_shape=(
            pltpu.VMEM((rows // nh, queries.shape[1] * nh), bf16),
            pltpu.VMEM((2 * group, rows), f32),
        ),
        in_specs=[pl.BlockSpec(memory_space=pl.ANY)] * 4,
        out_specs=(pl.BlockSpec(memory_space=pltpu.VMEM),) * 2,
        scratch_shapes=[
            pltpu.VMEM((2, high, head_dim), bf16),
            pltpu.VMEM((2, high, head_dim), bf16),
            pltpu.VMEM((2, PARTS, 2, rows // PARTS, head_dim), bf16),
            pltpu.VMEM((n, PARTS, 2, rows // PARTS, head_dim), bf16),
            pltpu.VMEM((2, high, rows), f32),
            pltpu.VMEM((2, high, rows), f32),
            pltpu.VMEM((2, high, head_dim), f32),
            pltpu.VMEM((2, rows, group * head_dim), bf16),
            pltpu.VMEM((2, 8, rows), f32),
            pltpu.VMEM((2, 8, rows), f32),
            pltpu.SMEM(block_order.shape, jnp.int32),
            dma((3,)),
            dma,
            dma,
            dma,
            dma((n, PARTS)),
            dma,
            dma((2,)),
            dma,
            dma,
            dma,
            dma,
            pltpu.SemaphoreType.REGULAR((n,)),
            pltpu.SemaphoreType.REGULAR,
        ],
        compiler_params=pltpu.CompilerParams(collective_id=0, has_side_effects=True),
    )(block_order, queries, keys, values)
    attn, lse = (pltpu.with_memory_space_constraint(z, pltpu.VMEM) for z in (attn, lse))
    return pl.pallas_call(
        hand_over,
        out_shape=(pltpu.HBM(attn.shape, bf16), pltpu.HBM(lse.shape, f32)),
        in_specs=[pl.BlockSpec(memory_space=pltpu.VMEM)] * 2,
        out_specs=(pl.BlockSpec(memory_space=pltpu.HBM),) * 2,
        scratch_shapes=[dma((2,))],
    )(attn, lse)


def solution(mesh):
    in_specs = (P("seq", "head"), P("seq", "head"), P("seq", "head"), P())
    out_specs = (P(("seq", "head"), None), P("head", "seq"))
    body = functools.partial(local, mesh.shape["seq"], mesh.shape["head"])
    return jax.shard_map(body, mesh=mesh, in_specs=in_specs, out_specs=out_specs, check_vma=False)
```

```python
import functools

import jax
import jax.numpy as jnp
from jax import lax
from jax.experimental import pallas as pl
from jax.experimental.pallas import tpu as pltpu
from jax.sharding import PartitionSpec as P

HEAD_SIZE = 256
QUERY_GROUP = 2
MASKED = -1e30
FLOOR = -1e20
PARTS = 1
TEAM = 4
MESH = pl.DeviceIdType.MESH


def loop(first, last, body):
    if last - first <= 8:
        for i in range(first, last):
            body(i)
    else:
        lax.fori_loop(first, last, lambda i, c: (body(i), c)[1], 0)


def kernel(
    n, nh, order_hbm, q_hbm, k_hbm, v_hbm, attn, lse,
    qbuf, qout, kvout, kvbuf, maxima, sums, accum, obuf, lse_tx, lse_rx, order,
    load_sem, cross_sem, near_sem, share_sem, kv_recv, q_send, q_recv,
    o_send, o_recv, l_send, l_recv, ready, plane_ready,
):
    head_dim, group = HEAD_SIZE, QUERY_GROUP
    rows = k_hbm.shape[0]
    keep = rows // nh
    part = rows // PARTS
    teams, planes = n // TEAM, nh // 2
    scale = head_dim ** (-0.5)
    width = group * head_dim
    me, h = lax.axis_index("seq"), lax.axis_index("head")
    x, c = h // 2, lax.rem(h, 2)
    g, j = me // TEAM, lax.rem(me, TEAM)
    y = lax.rem(j, 2)
    keeper = 1 - y
    own = c == keeper
    other = jnp.logical_not(own)
    base = 1 - c
    partner = x * 2 + 1 - c
    upper = j // 2

    def rank(m):
        return m // 2 + 2 * (m % 2)

    place = upper + 2 * y


    def lanes(start, size):
        return pl.ds(pl.multiple_of(start, head_dim), size)

    barrier = pltpu.get_barrier_semaphore()

    def signal(sem, s, hh):
        pl.semaphore_signal(sem, inc=1, device_id=(s, hh), device_id_type=MESH)

    for m in range(TEAM):
        @pl.when(rank(m) > place)
        def _():
            signal(barrier, g * TEAM + m, x * 2)
            signal(barrier, g * TEAM + m, x * 2 + 1)

    def greet_team(d):
        @pl.when(g + d < teams)
        def _():
            for i in range(2):
                signal(barrier, (g + d) * TEAM + base + 2 * i, x * 2 + 1)

            @pl.when(c == 1)
            def _():
                for m in range(TEAM):
                    signal(barrier, (g + d) * TEAM + m, x * 2 + keeper)

    loop(1, teams, greet_team)

    @pl.when(c == 0)
    def _():
        signal(barrier, me, partner)

    for xx in range(planes):
        @pl.when(xx > x)
        def _():
            signal(barrier, me, xx * 2 + c)

    def load(src, dst, i):
        pltpu.make_async_copy(src, dst, load_sem.at[i]).start()

    for i in range(2):
        for g2 in range(group):
            load(q_hbm.at[:, lanes((i * group + g2) * head_dim, head_dim)],
                 qout.at[i, pl.ds(g2 * rows, rows)], 0)
    for i in range(2):
        for t in range(PARTS):
            for z, src in enumerate((k_hbm, v_hbm)):
                load(src.at[pl.ds(t * part, part), lanes(i * head_dim, head_dim)],
                     kvout.at[i, t, z], 0)

    @pl.when(own)
    def _():
        for g2 in range(group):
            load(q_hbm.at[:, lanes((upper * group + g2) * head_dim, head_dim)],
                 qbuf.at[upper, pl.ds(g2 * rows, rows)], 1)
        for t in range(PARTS):
            for z, src in enumerate((k_hbm, v_hbm)):
                load(src.at[pl.ds(t * part, part), lanes(upper * head_dim, head_dim)],
                     kvbuf.at[me, t, z], 1)

    order_copy = pltpu.make_async_copy(order_hbm, order, load_sem.at[2])
    order_copy.start()

    def wait(sem, count):
        @pl.when(count > 0)
        def _():
            pl.semaphore_wait(sem, count)

    wait(barrier, 2 * place + c + x + g * (2 + 4 * c))

    for m in range(TEAM):
        @pl.when(rank(m) < place)
        def _():
            signal(ready.at[me], g * TEAM + m, x * 2)
            signal(ready.at[me], g * TEAM + m, x * 2 + 1)

    @pl.when(c == 1)
    def _():
        signal(ready.at[me], me, partner)

        def answer_team(d):
            @pl.when(g - d >= 0)
            def _():
                for m in range(TEAM):
                    signal(ready.at[me], (g - d) * TEAM + m, x * 2 + keeper)

        loop(1, teams, answer_team)

    def q_copy(i):
        return pltpu.make_async_remote_copy(
            src_ref=qout.at[i], dst_ref=qbuf.at[upper], send_sem=q_send, recv_sem=q_recv.at[upper],
            device_id=(g * TEAM + base + 2 * i, x * 2 + keeper), device_id_type=MESH)

    def kv_copy(i, t, team, core, sem):
        return pltpu.make_async_remote_copy(
            src_ref=kvout.at[i, t], dst_ref=kvbuf.at[me, t],
            send_sem=sem, recv_sem=kv_recv.at[me, t],
            device_id=(team * TEAM + base + 2 * i, x * 2 + core), device_id_type=MESH)

    def share(slot, t):
        return pltpu.make_async_remote_copy(
            src_ref=kvbuf.at[slot, t], dst_ref=kvbuf.at[slot, t],
            send_sem=share_sem, recv_sem=kv_recv.at[slot, t],
            device_id=(me, partner), device_id_type=MESH)

    def ask(i):
        q_copy(i).start()

    def near(i):
        for t in range(PARTS):
            kv_copy(i, t, g, 1, near_sem).start()

    def cross(team, turn):
        for i in turn:
            for t in range(PARTS):
                kv_copy(i, t, team, 1, cross_sem).start()

    for i, whole in ((0, (qout, kvout)), ):
        for z in whole:
            pltpu.make_async_copy(z, z, load_sem.at[i]).wait()

    pair = [upper, 1 - upper]
    spot = [i + 2 * base for i in pair]

    def cross_back(d):
        @pl.when(g - d >= 0)
        def _():
            cross(g - d, (0, 1))

    def cross_on(d):
        @pl.when(g + d < teams)
        def _():
            for i in range(2):
                pl.semaphore_wait(ready.at[(g + d) * TEAM + base + 2 * i], 1)
            cross(g + d, (1, 0))

    def ask_both():
        for i, r in zip(pair, spot):
            @pl.when(r > place)
            def _():
                pl.semaphore_wait(ready.at[g * TEAM + base + 2 * i], 2)

            pl.when(r != place)(functools.partial(ask, i))

    pl.when(spot[1] < place)(ask_both)
    loop(1, teams, cross_back)
    pl.when(spot[1] >= place)(ask_both)
    for i, r in zip(pair, spot):
        pl.when(r != place)(functools.partial(near, i))

    @pl.when(c == 0)
    def _():
        pl.semaphore_wait(ready.at[me], 1)

    @pl.when(own)
    def _():
        for z in (qbuf.at[0], kvbuf.at[0]):
            pltpu.make_async_copy(z, z, load_sem.at[1]).wait()
        for t in range(PARTS):
            share(me, t).start()

    loop(1, teams, cross_on)

    maxima[...] = jnp.full_like(maxima, FLOOR)
    sums[...] = jnp.zeros_like(sums)
    accum[...] = jnp.zeros_like(accum)
    order_copy.wait()

    row = lax.broadcasted_iota(jnp.int32, (rows, rows), 0)
    col = lax.broadcasted_iota(jnp.int32, (rows, rows), 1)
    per = order.shape[0] // n
    blk = rows // per

    def placed(index, s):
        out = index + order[s * per] * blk
        for b in range(1, per):
            out = jnp.where(index >= b * blk, index + (order[s * per + b] - b) * blk, out)
        return out

    query_pos = [placed(row, g * TEAM + base + 2 * rs) for rs in range(2)]

    def fold(z):
        return z.reshape(rows, head_dim)

    def attend(parts, slots):
        for rs in parts:
            scores = []
            for slot in slots:
                one = lax.dot_general(
                    qbuf[rs], fold(kvbuf[slot, :, 0]), (((1,), (1,)), ((), ())),
                    preferred_element_type=jnp.float32) * scale
                allowed = placed(col, slot) <= query_pos[rs]
                scores.append(jnp.where(jnp.concatenate([allowed] * group, 0), one, MASKED))
            before = maxima[rs]
            top = functools.reduce(jnp.maximum, scores)
            fresh = jnp.maximum(before, jnp.max(top, axis=1, keepdims=True))
            factor = jnp.exp(before - fresh)
            maxima[rs] = fresh
            weights = [jnp.exp(one - fresh) for one in scores]
            sums[rs] = sums[rs] * factor + functools.reduce(jnp.add, weights)
            update = [
                lax.dot_general(
                    w.astype(jnp.bfloat16), fold(kvbuf[slot, :, 1]), (((1,), (0,)), ((), ())),
                    preferred_element_type=jnp.float32)
                for w, slot in zip(weights, slots)]
            accum[rs] = accum[rs] * jnp.concatenate(
                [factor] * (head_dim // rows), 1) + functools.reduce(jnp.add, update)

    def landed(slot, t):
        share(slot, t).wait_recv()

    def take(slot):
        for t in range(PARTS):
            landed(slot, t)

            @pl.when(c == 1)
            def _():
                share(slot, t).start()
        return slot

    @pl.when(other)
    def _():
        for t in range(PARTS):
            landed(me, t)

    for rs in range(2):
        @pl.when(other | (upper != rs))
        def _():
            pltpu.make_async_remote_copy(
                src_ref=qout.at[0], dst_ref=qbuf.at[rs], send_sem=q_send,
                recv_sem=q_recv.at[rs], device_id=(me, partner), device_id_type=MESH).wait_recv()

    attend((0, 1), (me,))

    beside = g * TEAM + j + 1 - 2 * y
    above = g * TEAM + lax.rem(j + 2, TEAM)
    across = above + 1 - 2 * y
    for m in range(TEAM):
        @pl.when((m % 2 == c) & (rank(m) > place))
        def _():
            pl.semaphore_wait(ready.at[g * TEAM + m], 2)

    for xx in range(planes):
        @pl.when(xx < x)
        def _():
            signal(plane_ready, me, xx * 2 + c)

    both = (0, 1)
    if teams == 2:
        there = (1 - g) * TEAM
        close = (above, across)
        lead = 2 * upper
        far = [there + lead, there + lead + 1, there + 2 - lead, there + 3 - lead]


        attend(both, (take(beside),))
        lower = g == 0
        stages = [(jnp.where(lower, a, b), jnp.where(lower, b, d), jnp.where(lower, d, a))
                  for a, b, d in zip(close, far[:2], far[2:])]
        first, second, final = zip(*stages)
        attend(both, [take(s) for s in first])
        wait(plane_ready, planes - 1 - x)

        for xx in range(planes):
            @pl.when(xx > x)
            def _():
                signal(plane_ready, me, xx * 2 + c)

        attend(both, [take(s) for s in second])
        for s in final:
            take(s)
    else:
        attend(both, [take(s) for s in (beside, above, across)])
        wait(plane_ready, planes - 1 - x)

        for xx in range(planes):
            @pl.when(xx > x)
            def _():
                signal(plane_ready, me, xx * 2 + c)

        def slot_of(k):
            return lax.rem(g + 1 + k // TEAM, teams) * TEAM + lax.rem(k, TEAM)

        def further(k):
            attend(both, (take(slot_of(jnp.int32(k))),))

        loop(0, TEAM * (teams - 1) - 1, further)
        final = [slot_of(jnp.int32(TEAM * (teams - 1) - 1))]
        take(final[0])

    def finish(rs):
        total = jnp.sum(sums[rs], axis=1, keepdims=True)
        out = (accum[rs] / total).astype(jnp.bfloat16)
        for g2 in range(group):
            obuf[rs, :, g2 * head_dim:(g2 + 1) * head_dim] = out[g2 * rows:(g2 + 1) * rows]
        return jnp.log(total) + maxima[rs]

    columns = lanes(((x * 2 + keeper) * 2 + upper) * width, width)
    wait(plane_ready, x)

    def send_out(rs, k):
        mine = own & (upper == rs)
        to = lax.rem(x + 1 + k, planes) * 2 + lax.rem(c + 1 + k // planes, 2)
        src = obuf.at[rs, pl.ds(pl.multiple_of(to * keep, keep), keep)]

        def away():
            pltpu.make_async_remote_copy(
                src_ref=src, dst_ref=attn.at[:, columns], send_sem=o_send, recv_sem=o_recv,
                device_id=(g * TEAM + base + 2 * rs, to), device_id_type=MESH).start()

        if k < nh - 1:
            away()
        else:
            pl.when(jnp.logical_not(mine))(away)

            @pl.when(mine)
            def _():
                pltpu.make_async_copy(src, attn.at[:, columns], o_send).start()

    def send_lse(rs, full):
        for g2 in range(group):
            lse_tx[rs, g2:g2 + 1, :] = jnp.transpose(full[g2 * rows:(g2 + 1) * rows])[:1]
        mine = own & (upper == rs)

        @pl.when(jnp.logical_not(mine))
        def _():
            pltpu.make_async_remote_copy(
                src_ref=lse_tx.at[rs], dst_ref=lse_rx.at[upper], send_sem=l_send, recv_sem=l_recv,
                device_id=(g * TEAM + base + 2 * rs, x * 2 + keeper), device_id_type=MESH).start()

        @pl.when(mine)
        def _():
            lse_rx[rs] = lse_tx[rs]

    attend(both, final)
    fulls = [finish(0), finish(1)]
    for k in range(nh):
        for rs in (1 - upper, upper):
            send_out(rs, k)
        if k == 1:
            for rs in range(2):
                send_lse(rs, fulls[rs])

    def drain(ref, sem):
        pltpu.make_async_copy(ref, ref, sem).wait()

    def by_kind(ref, less, sem):
        pl.when(own)(lambda: drain(less, sem))
        pl.when(other)(lambda: drain(ref, sem))

    by_kind(lse_rx, lse_rx.at[pl.ds(0, 1)], l_recv)
    lse[...] = jnp.concatenate([lse_rx[0, :group], lse_rx[1, :group]], 0)
    by_kind(attn, attn.at[:, pl.ds(0, (2 * nh - 1) * width)], o_recv)
    drain(attn, o_send)
    by_kind(lse_tx, lse_tx.at[pl.ds(0, 1)], l_send)
    by_kind(qbuf, qbuf.at[pl.ds(0, 1)], q_send)
    by_kind(kvbuf.at[pl.ds(0, 2)], kvbuf.at[pl.ds(0, 1)], near_sem)
    drain(kvbuf.at[pl.ds(0, 2 * (teams - 1))], cross_sem)
    pl.when((c == 1) & own)(functools.partial(drain, kvbuf, share_sem))
    pl.when((c == 1) & other)(functools.partial(drain, kvbuf.at[pl.ds(0, n - 1)], share_sem))
    pl.when((c == 0) & own)(functools.partial(drain, kvbuf.at[0], share_sem))


def hand_over(attn, lse, attn_hbm, lse_hbm, sem):
    copies = [
        pltpu.make_async_copy(attn, attn_hbm, sem.at[0]),
        pltpu.make_async_copy(lse, lse_hbm, sem.at[1]),
    ]
    for c in copies:
        c.start()
    for c in copies:
        c.wait()


def local(n, nh, queries, keys, values, block_order):
    rows = queries.shape[0]
    head_dim, group = HEAD_SIZE, QUERY_GROUP
    high = group * rows
    bf16, f32 = jnp.bfloat16, jnp.float32
    dma = pltpu.SemaphoreType.DMA
    attn, lse = pl.pallas_call(
        functools.partial(kernel, n, nh),
        out_shape=(
            pltpu.VMEM((rows // nh, queries.shape[1] * nh), bf16),
            pltpu.VMEM((2 * group, rows), f32),
        ),
        in_specs=[pl.BlockSpec(memory_space=pl.ANY)] * 4,
        out_specs=(pl.BlockSpec(memory_space=pltpu.VMEM),) * 2,
        scratch_shapes=[
            pltpu.VMEM((2, high, head_dim), bf16),
            pltpu.VMEM((2, high, head_dim), bf16),
            pltpu.VMEM((2, PARTS, 2, rows // PARTS, head_dim), bf16),
            pltpu.VMEM((n, PARTS, 2, rows // PARTS, head_dim), bf16),
            pltpu.VMEM((2, high, rows), f32),
            pltpu.VMEM((2, high, rows), f32),
            pltpu.VMEM((2, high, head_dim), f32),
            pltpu.VMEM((2, rows, group * head_dim), bf16),
            pltpu.VMEM((2, 8, rows), f32),
            pltpu.VMEM((2, 8, rows), f32),
            pltpu.SMEM(block_order.shape, jnp.int32),
            dma((3,)),
            dma,
            dma,
            dma,
            dma((n, PARTS)),
            dma,
            dma((2,)),
            dma,
            dma,
            dma,
            dma,
            pltpu.SemaphoreType.REGULAR((n,)),
            pltpu.SemaphoreType.REGULAR,
        ],
        compiler_params=pltpu.CompilerParams(collective_id=0, has_side_effects=True),
    )(block_order, queries, keys, values)
    attn, lse = (pltpu.with_memory_space_constraint(z, pltpu.VMEM) for z in (attn, lse))
    return pl.pallas_call(
        hand_over,
        out_shape=(pltpu.HBM(attn.shape, bf16), pltpu.HBM(lse.shape, f32)),
        in_specs=[pl.BlockSpec(memory_space=pltpu.VMEM)] * 2,
        out_specs=(pl.BlockSpec(memory_space=pltpu.HBM),) * 2,
        scratch_shapes=[dma((2,))],
    )(attn, lse)


def solution(mesh):
    in_specs = (P("seq", "head"), P("seq", "head"), P("seq", "head"), P())
    out_specs = (P(("seq", "head"), None), P("head", "seq"))
    body = functools.partial(local, mesh.shape["seq"], mesh.shape["head"])
    return jax.shard_map(body, mesh=mesh, in_specs=in_specs, out_specs=out_specs, check_vma=False)
```

```python
import functools

import jax
import jax.numpy as jnp
from jax import lax
from jax.experimental import pallas as pl
from jax.experimental.pallas import tpu as pltpu
from jax.sharding import PartitionSpec as P

HEAD_SIZE = 256
QUERY_GROUP = 2
MASKED = -1e30
FLOOR = -1e20
PARTS = 2
LEAD = 1
TEAM = 4
MESH = pl.DeviceIdType.MESH


def loop(first, last, body):
    if last - first <= 8:
        for i in range(first, last):
            body(i)
    else:
        lax.fori_loop(first, last, lambda i, c: (body(i), c)[1], 0)


def kernel(
    n, nh, order_hbm, q_hbm, k_hbm, v_hbm, attn, lse,
    qbuf, qout, kvout, kvbuf, maxima, sums, accum, obuf, lse_tx, lse_rx, order,
    load_sem, cross_sem, near_sem, share_sem, kv_recv, q_send, q_recv,
    o_send, o_recv, l_send, l_recv, ready, plane_ready,
):
    head_dim, group = HEAD_SIZE, QUERY_GROUP
    rows = k_hbm.shape[0]
    keep = rows // nh
    part = rows // PARTS
    teams, planes = n // TEAM, nh // 2
    scale = head_dim ** (-0.5)
    width = group * head_dim
    me, h = lax.axis_index("seq"), lax.axis_index("head")
    x, c = h // 2, lax.rem(h, 2)
    g, j = me // TEAM, lax.rem(me, TEAM)
    y = lax.rem(j, 2)
    keeper = 1 - y
    own = c == keeper
    other = jnp.logical_not(own)
    base = 1 - c
    partner = x * 2 + 1 - c
    upper = j // 2

    def rank(m):
        return m // 2 + 2 * (m % 2)

    place = upper + 2 * y


    def lanes(start, size):
        return pl.ds(pl.multiple_of(start, head_dim), size)

    barrier = pltpu.get_barrier_semaphore()

    def signal(sem, s, hh):
        pl.semaphore_signal(sem, inc=1, device_id=(s, hh), device_id_type=MESH)

    for m in range(TEAM):
        @pl.when(rank(m) > place)
        def _():
            signal(barrier, g * TEAM + m, x * 2)
            signal(barrier, g * TEAM + m, x * 2 + 1)

    def greet_team(d):
        @pl.when(g + d < teams)
        def _():
            for i in range(2):
                signal(barrier, (g + d) * TEAM + base + 2 * i, x * 2 + 1)

            @pl.when(c == 1)
            def _():
                for m in range(TEAM):
                    signal(barrier, (g + d) * TEAM + m, x * 2 + keeper)

    loop(1, teams, greet_team)

    @pl.when(c == 0)
    def _():
        signal(barrier, me, partner)

    for xx in range(planes):
        @pl.when(xx > x)
        def _():
            signal(barrier, me, xx * 2 + c)

    def load(src, dst, i):
        pltpu.make_async_copy(src, dst, load_sem.at[i]).start()

    for i in range(2):
        for g2 in range(group):
            load(q_hbm.at[:, lanes((i * group + g2) * head_dim, head_dim)],
                 qout.at[i, pl.ds(g2 * rows, rows)], 0)
    for i in range(2):
        for t in range(PARTS):
            for z, src in enumerate((k_hbm, v_hbm)):
                load(src.at[pl.ds(t * part, part), lanes(i * head_dim, head_dim)],
                     kvout.at[i, t, z], 0)

    @pl.when(own)
    def _():
        for g2 in range(group):
            load(q_hbm.at[:, lanes((upper * group + g2) * head_dim, head_dim)],
                 qbuf.at[upper, pl.ds(g2 * rows, rows)], 1)
        for t in range(PARTS):
            for z, src in enumerate((k_hbm, v_hbm)):
                load(src.at[pl.ds(t * part, part), lanes(upper * head_dim, head_dim)],
                     kvbuf.at[me, t, z], 1)

    order_copy = pltpu.make_async_copy(order_hbm, order, load_sem.at[2])
    order_copy.start()

    def wait(sem, count):
        @pl.when(count > 0)
        def _():
            pl.semaphore_wait(sem, count)

    wait(barrier, 2 * place + c + x + g * (2 + 4 * c))

    for m in range(TEAM):
        @pl.when(rank(m) < place)
        def _():
            signal(ready.at[me], g * TEAM + m, x * 2)
            signal(ready.at[me], g * TEAM + m, x * 2 + 1)

    @pl.when(c == 1)
    def _():
        signal(ready.at[me], me, partner)

        def answer_team(d):
            @pl.when(g - d >= 0)
            def _():
                for m in range(TEAM):
                    signal(ready.at[me], (g - d) * TEAM + m, x * 2 + keeper)

        loop(1, teams, answer_team)

    def q_copy(i):
        return pltpu.make_async_remote_copy(
            src_ref=qout.at[i], dst_ref=qbuf.at[upper], send_sem=q_send, recv_sem=q_recv.at[upper],
            device_id=(g * TEAM + base + 2 * i, x * 2 + keeper), device_id_type=MESH)

    def kv_copy(i, t, team, core, sem):
        return pltpu.make_async_remote_copy(
            src_ref=kvout.at[i, t], dst_ref=kvbuf.at[me, t],
            send_sem=sem, recv_sem=kv_recv.at[me, t],
            device_id=(team * TEAM + base + 2 * i, x * 2 + core), device_id_type=MESH)

    def share(slot, t):
        return pltpu.make_async_remote_copy(
            src_ref=kvbuf.at[slot, t], dst_ref=kvbuf.at[slot, t],
            send_sem=share_sem, recv_sem=kv_recv.at[slot, t],
            device_id=(me, partner), device_id_type=MESH)

    def ask(i):
        q_copy(i).start()

    def near(i):
        for t in range(PARTS):
            kv_copy(i, t, g, 1, near_sem).start()

    def cross(team, turn):
        for i in turn:
            for t in range(PARTS):
                kv_copy(i, t, team, 1, cross_sem).start()

    for i, whole in ((0, (qout, kvout)), ):
        for z in whole:
            pltpu.make_async_copy(z, z, load_sem.at[i]).wait()

    pair = [upper, 1 - upper]
    spot = [i + 2 * base for i in pair]

    def cross_back(d):
        @pl.when(g - d >= 0)
        def _():
            cross(g - d, (0, 1))

    def cross_on(d):
        @pl.when(g + d < teams)
        def _():
            for i, spans in ((0, range(LEAD)), (1, range(PARTS)), (0, range(LEAD, PARTS))):
                if spans.start == 0:
                    pl.semaphore_wait(ready.at[(g + d) * TEAM + base + 2 * i], 1)
                for t in spans:
                    kv_copy(i, t, g + d, 1, cross_sem).start()

    def ask_both():
        for i, r in zip(pair, spot):
            @pl.when(r > place)
            def _():
                pl.semaphore_wait(ready.at[g * TEAM + base + 2 * i], 2)

            pl.when(r != place)(functools.partial(ask, i))

    pl.when(spot[1] < place)(ask_both)
    loop(1, teams, cross_back)
    pl.when(spot[1] >= place)(ask_both)
    for i, r in zip(pair, spot):
        pl.when(r != place)(functools.partial(near, i))

    @pl.when(c == 0)
    def _():
        pl.semaphore_wait(ready.at[me], 1)

    @pl.when(own)
    def _():
        for z in (qbuf.at[0], kvbuf.at[0]):
            pltpu.make_async_copy(z, z, load_sem.at[1]).wait()
        for t in range(PARTS):
            share(me, t).start()

    loop(1, teams, cross_on)

    maxima[...] = jnp.full_like(maxima, FLOOR)
    sums[...] = jnp.zeros_like(sums)
    accum[...] = jnp.zeros_like(accum)
    order_copy.wait()

    row = lax.broadcasted_iota(jnp.int32, (rows, rows), 0)
    col = lax.broadcasted_iota(jnp.int32, (rows, rows), 1)
    per = order.shape[0] // n
    blk = rows // per

    def placed(index, s):
        out = index + order[s * per] * blk
        for b in range(1, per):
            out = jnp.where(index >= b * blk, index + (order[s * per + b] - b) * blk, out)
        return out

    query_pos = [placed(row, g * TEAM + base + 2 * rs) for rs in range(2)]

    def fold(z):
        return z.reshape(rows, head_dim)

    def attend(parts, slots):
        for rs in parts:
            scores = []
            for slot in slots:
                one = lax.dot_general(
                    qbuf[rs], fold(kvbuf[slot, :, 0]), (((1,), (1,)), ((), ())),
                    preferred_element_type=jnp.float32) * scale
                allowed = placed(col, slot) <= query_pos[rs]
                scores.append(jnp.where(jnp.concatenate([allowed] * group, 0), one, MASKED))
            before = maxima[rs]
            top = functools.reduce(jnp.maximum, scores)
            fresh = jnp.maximum(before, jnp.max(top, axis=1, keepdims=True))
            factor = jnp.exp(before - fresh)
            maxima[rs] = fresh
            weights = [jnp.exp(one - fresh) for one in scores]
            sums[rs] = sums[rs] * factor + functools.reduce(jnp.add, weights)
            update = [
                lax.dot_general(
                    w.astype(jnp.bfloat16), fold(kvbuf[slot, :, 1]), (((1,), (0,)), ((), ())),
                    preferred_element_type=jnp.float32)
                for w, slot in zip(weights, slots)]
            accum[rs] = accum[rs] * jnp.concatenate(
                [factor] * (head_dim // rows), 1) + functools.reduce(jnp.add, update)

    def landed(slot, t):
        share(slot, t).wait_recv()

    def take(slot):
        for t in range(PARTS):
            landed(slot, t)

            @pl.when(c == 1)
            def _():
                share(slot, t).start()
        return slot

    @pl.when(other)
    def _():
        for t in range(PARTS):
            landed(me, t)

    for rs in range(2):
        @pl.when(other | (upper != rs))
        def _():
            pltpu.make_async_remote_copy(
                src_ref=qout.at[0], dst_ref=qbuf.at[rs], send_sem=q_send,
                recv_sem=q_recv.at[rs], device_id=(me, partner), device_id_type=MESH).wait_recv()

    attend((0, 1), (me,))

    beside = g * TEAM + j + 1 - 2 * y
    above = g * TEAM + lax.rem(j + 2, TEAM)
    across = above + 1 - 2 * y
    for m in range(TEAM):
        @pl.when((m % 2 == c) & (rank(m) > place))
        def _():
            pl.semaphore_wait(ready.at[g * TEAM + m], 2)

    for xx in range(planes):
        @pl.when(xx < x)
        def _():
            signal(plane_ready, me, xx * 2 + c)

    both = (0, 1)
    if teams == 2:
        there = (1 - g) * TEAM
        close = (above, across)
        lead = 2 * upper
        far = [there + lead, there + lead + 1, there + 2 - lead, there + 3 - lead]


        attend(both, (take(beside),))
        low, up = g == 0, upper == 1
        stages = [
            (jnp.where(low & up, a, b),
             jnp.where(low & up, b, jnp.where(low | up, d, a)),
             jnp.where(low == up, d, a))
            for a, b, d in zip(close, far[:2], far[2:])]
        first, second, final = zip(*stages)
        attend(both, [take(s) for s in first])
        wait(plane_ready, planes - 1 - x)

        for xx in range(planes):
            @pl.when(xx > x)
            def _():
                signal(plane_ready, me, xx * 2 + c)

        attend(both, [take(s) for s in second])
        for s in final:
            take(s)
    else:
        attend(both, [take(s) for s in (beside, above, across)])
        wait(plane_ready, planes - 1 - x)

        for xx in range(planes):
            @pl.when(xx > x)
            def _():
                signal(plane_ready, me, xx * 2 + c)

        def slot_of(k):
            return lax.rem(g + 1 + k // TEAM, teams) * TEAM + lax.rem(k, TEAM)

        def further(k):
            attend(both, (take(slot_of(jnp.int32(k))),))

        loop(0, TEAM * (teams - 1) - 1, further)
        final = [slot_of(jnp.int32(TEAM * (teams - 1) - 1))]
        take(final[0])

    def finish(rs):
        total = jnp.sum(sums[rs], axis=1, keepdims=True)
        out = (accum[rs] / total).astype(jnp.bfloat16)
        for g2 in range(group):
            obuf[rs, :, g2 * head_dim:(g2 + 1) * head_dim] = out[g2 * rows:(g2 + 1) * rows]
        return jnp.log(total) + maxima[rs]

    columns = lanes(((x * 2 + keeper) * 2 + upper) * width, width)
    wait(plane_ready, x)

    def send_out(rs, k):
        mine = own & (upper == rs)
        to = lax.rem(x + 1 + k, planes) * 2 + lax.rem(c + 1 + k // planes, 2)
        src = obuf.at[rs, pl.ds(pl.multiple_of(to * keep, keep), keep)]

        def away():
            pltpu.make_async_remote_copy(
                src_ref=src, dst_ref=attn.at[:, columns], send_sem=o_send, recv_sem=o_recv,
                device_id=(g * TEAM + base + 2 * rs, to), device_id_type=MESH).start()

        if k < nh - 1:
            away()
        else:
            pl.when(jnp.logical_not(mine))(away)

            @pl.when(mine)
            def _():
                pltpu.make_async_copy(src, attn.at[:, columns], o_send).start()

    def send_lse(rs, full):
        for g2 in range(group):
            lse_tx[rs, g2:g2 + 1, :] = jnp.transpose(full[g2 * rows:(g2 + 1) * rows])[:1]
        mine = own & (upper == rs)

        @pl.when(jnp.logical_not(mine))
        def _():
            pltpu.make_async_remote_copy(
                src_ref=lse_tx.at[rs], dst_ref=lse_rx.at[upper], send_sem=l_send, recv_sem=l_recv,
                device_id=(g * TEAM + base + 2 * rs, x * 2 + keeper), device_id_type=MESH).start()

        @pl.when(mine)
        def _():
            lse_rx[rs] = lse_tx[rs]

    attend(both, final)
    for rs in (1 - upper, upper):
        full = finish(rs)
        for k in range(nh):
            send_out(rs, k)
        send_lse(rs, full)

    def drain(ref, sem):
        pltpu.make_async_copy(ref, ref, sem).wait()

    def by_kind(ref, less, sem):
        pl.when(own)(lambda: drain(less, sem))
        pl.when(other)(lambda: drain(ref, sem))

    by_kind(lse_rx, lse_rx.at[pl.ds(0, 1)], l_recv)
    lse[...] = jnp.concatenate([lse_rx[0, :group], lse_rx[1, :group]], 0)
    by_kind(attn, attn.at[:, pl.ds(0, (2 * nh - 1) * width)], o_recv)
    drain(attn, o_send)
    by_kind(lse_tx, lse_tx.at[pl.ds(0, 1)], l_send)
    by_kind(qbuf, qbuf.at[pl.ds(0, 1)], q_send)
    by_kind(kvbuf.at[pl.ds(0, 2)], kvbuf.at[pl.ds(0, 1)], near_sem)
    drain(kvbuf.at[pl.ds(0, 2 * (teams - 1))], cross_sem)
    pl.when((c == 1) & own)(functools.partial(drain, kvbuf, share_sem))
    pl.when((c == 1) & other)(functools.partial(drain, kvbuf.at[pl.ds(0, n - 1)], share_sem))
    pl.when((c == 0) & own)(functools.partial(drain, kvbuf.at[0], share_sem))


def hand_over(attn, lse, attn_hbm, lse_hbm, sem):
    copies = [
        pltpu.make_async_copy(attn, attn_hbm, sem.at[0]),
        pltpu.make_async_copy(lse, lse_hbm, sem.at[1]),
    ]
    for c in copies:
        c.start()
    for c in copies:
        c.wait()


def local(n, nh, queries, keys, values, block_order):
    rows = queries.shape[0]
    head_dim, group = HEAD_SIZE, QUERY_GROUP
    high = group * rows
    bf16, f32 = jnp.bfloat16, jnp.float32
    dma = pltpu.SemaphoreType.DMA
    attn, lse = pl.pallas_call(
        functools.partial(kernel, n, nh),
        out_shape=(
            pltpu.VMEM((rows // nh, queries.shape[1] * nh), bf16),
            pltpu.VMEM((2 * group, rows), f32),
        ),
        in_specs=[pl.BlockSpec(memory_space=pl.ANY)] * 4,
        out_specs=(pl.BlockSpec(memory_space=pltpu.VMEM),) * 2,
        scratch_shapes=[
            pltpu.VMEM((2, high, head_dim), bf16),
            pltpu.VMEM((2, high, head_dim), bf16),
            pltpu.VMEM((2, PARTS, 2, rows // PARTS, head_dim), bf16),
            pltpu.VMEM((n, PARTS, 2, rows // PARTS, head_dim), bf16),
            pltpu.VMEM((2, high, rows), f32),
            pltpu.VMEM((2, high, rows), f32),
            pltpu.VMEM((2, high, head_dim), f32),
            pltpu.VMEM((2, rows, group * head_dim), bf16),
            pltpu.VMEM((2, 8, rows), f32),
            pltpu.VMEM((2, 8, rows), f32),
            pltpu.SMEM(block_order.shape, jnp.int32),
            dma((3,)),
            dma,
            dma,
            dma,
            dma((n, PARTS)),
            dma,
            dma((2,)),
            dma,
            dma,
            dma,
            dma,
            pltpu.SemaphoreType.REGULAR((n,)),
            pltpu.SemaphoreType.REGULAR,
        ],
        compiler_params=pltpu.CompilerParams(collective_id=0, has_side_effects=True),
    )(block_order, queries, keys, values)
    attn, lse = (pltpu.with_memory_space_constraint(z, pltpu.VMEM) for z in (attn, lse))
    return pl.pallas_call(
        hand_over,
        out_shape=(pltpu.HBM(attn.shape, bf16), pltpu.HBM(lse.shape, f32)),
        in_specs=[pl.BlockSpec(memory_space=pltpu.VMEM)] * 2,
        out_specs=(pl.BlockSpec(memory_space=pltpu.HBM),) * 2,
        scratch_shapes=[dma((2,))],
    )(attn, lse)


def solution(mesh):
    in_specs = (P("seq", "head"), P("seq", "head"), P("seq", "head"), P())
    out_specs = (P(("seq", "head"), None), P("head", "seq"))
    body = functools.partial(local, mesh.shape["seq"], mesh.shape["head"])
    return jax.shard_map(body, mesh=mesh, in_specs=in_specs, out_specs=out_specs, check_vma=False)
```

```python
import functools

import jax
import jax.numpy as jnp
from jax import lax
from jax.experimental import pallas as pl
from jax.experimental.pallas import tpu as pltpu
from jax.sharding import PartitionSpec as P

HEAD_SIZE = 256
QUERY_GROUP = 2
MASKED = -1e30
FLOOR = -1e20
PARTS = 2
LEAD = 1
TEAM = 4
MESH = pl.DeviceIdType.MESH


def loop(first, last, body):
    if last - first <= 8:
        for i in range(first, last):
            body(i)
    else:
        lax.fori_loop(first, last, lambda i, c: (body(i), c)[1], 0)


def kernel(
    n, nh, order_hbm, q_hbm, k_hbm, v_hbm, attn, lse,
    qbuf, qout, kvout, kvbuf, maxima, sums, accum, obuf, lse_tx, lse_rx, order,
    load_sem, cross_sem, near_sem, share_sem, kv_recv, q_send, q_recv,
    o_send, o_recv, l_send, l_recv, ready, plane_ready,
):
    head_dim, group = HEAD_SIZE, QUERY_GROUP
    rows = k_hbm.shape[0]
    keep = rows // nh
    part = rows // PARTS
    teams, planes = n // TEAM, nh // 2
    scale = head_dim ** (-0.5)
    width = group * head_dim
    me, h = lax.axis_index("seq"), lax.axis_index("head")
    x, c = h // 2, lax.rem(h, 2)
    g, j = me // TEAM, lax.rem(me, TEAM)
    y = lax.rem(j, 2)
    keeper = 1 - y
    own = c == keeper
    other = jnp.logical_not(own)
    base = 1 - c
    partner = x * 2 + 1 - c
    upper = j // 2

    def rank(m):
        return m // 2 + 2 * (m % 2)

    place = upper + 2 * y


    def lanes(start, size):
        return pl.ds(pl.multiple_of(start, head_dim), size)

    barrier = pltpu.get_barrier_semaphore()

    def signal(sem, s, hh):
        pl.semaphore_signal(sem, inc=1, device_id=(s, hh), device_id_type=MESH)

    for m in range(TEAM):
        @pl.when(rank(m) > place)
        def _():
            signal(barrier, g * TEAM + m, x * 2)
            signal(barrier, g * TEAM + m, x * 2 + 1)

    def greet_team(d):
        @pl.when(g + d < teams)
        def _():
            for i in range(2):
                signal(barrier, (g + d) * TEAM + base + 2 * i, x * 2 + 1)

            @pl.when(c == 1)
            def _():
                for m in range(TEAM):
                    signal(barrier, (g + d) * TEAM + m, x * 2 + keeper)

    loop(1, teams, greet_team)

    @pl.when(c == 0)
    def _():
        signal(barrier, me, partner)

    for xx in range(planes):
        @pl.when(xx > x)
        def _():
            signal(barrier, me, xx * 2 + c)

    def load(src, dst, i):
        pltpu.make_async_copy(src, dst, load_sem.at[i]).start()

    for i in range(2):
        for g2 in range(group):
            load(q_hbm.at[:, lanes((i * group + g2) * head_dim, head_dim)],
                 qout.at[i, pl.ds(g2 * rows, rows)], 0)
    for i in range(2):
        for t in range(PARTS):
            for z, src in enumerate((k_hbm, v_hbm)):
                load(src.at[pl.ds(t * part, part), lanes(i * head_dim, head_dim)],
                     kvout.at[i, t, z], 0)

    @pl.when(own)
    def _():
        for g2 in range(group):
            load(q_hbm.at[:, lanes((upper * group + g2) * head_dim, head_dim)],
                 qbuf.at[upper, pl.ds(g2 * rows, rows)], 1)
        for t in range(PARTS):
            for z, src in enumerate((k_hbm, v_hbm)):
                load(src.at[pl.ds(t * part, part), lanes(upper * head_dim, head_dim)],
                     kvbuf.at[me, t, z], 1)

    order_copy = pltpu.make_async_copy(order_hbm, order, load_sem.at[2])
    order_copy.start()

    def wait(sem, count):
        @pl.when(count > 0)
        def _():
            pl.semaphore_wait(sem, count)

    wait(barrier, 2 * place + c + x + g * (2 + 4 * c))

    for m in range(TEAM):
        @pl.when(rank(m) < place)
        def _():
            signal(ready.at[me], g * TEAM + m, x * 2)
            signal(ready.at[me], g * TEAM + m, x * 2 + 1)

    @pl.when(c == 1)
    def _():
        signal(ready.at[me], me, partner)

        def answer_team(d):
            @pl.when(g - d >= 0)
            def _():
                for m in range(TEAM):
                    signal(ready.at[me], (g - d) * TEAM + m, x * 2 + keeper)

        loop(1, teams, answer_team)

    def q_copy(i):
        return pltpu.make_async_remote_copy(
            src_ref=qout.at[i], dst_ref=qbuf.at[upper], send_sem=q_send, recv_sem=q_recv.at[upper],
            device_id=(g * TEAM + base + 2 * i, x * 2 + keeper), device_id_type=MESH)

    def kv_copy(i, t, team, core, sem):
        return pltpu.make_async_remote_copy(
            src_ref=kvout.at[i, t], dst_ref=kvbuf.at[me, t],
            send_sem=sem, recv_sem=kv_recv.at[me, t],
            device_id=(team * TEAM + base + 2 * i, x * 2 + core), device_id_type=MESH)

    def share(slot, t):
        return pltpu.make_async_remote_copy(
            src_ref=kvbuf.at[slot, t], dst_ref=kvbuf.at[slot, t],
            send_sem=share_sem, recv_sem=kv_recv.at[slot, t],
            device_id=(me, partner), device_id_type=MESH)

    def ask(i):
        q_copy(i).start()

    def near(i):
        for t in range(PARTS):
            kv_copy(i, t, g, 1, near_sem).start()

    def cross(team, turn):
        for i in turn:
            for t in range(PARTS):
                kv_copy(i, t, team, 1, cross_sem).start()

    for i, whole in ((0, (qout, kvout)), ):
        for z in whole:
            pltpu.make_async_copy(z, z, load_sem.at[i]).wait()

    pair = [upper, 1 - upper]
    spot = [i + 2 * base for i in pair]

    def cross_back(d):
        @pl.when(g - d >= 0)
        def _():
            cross(g - d, (0, 1))

    def cross_on(d):
        @pl.when(g + d < teams)
        def _():
            for i, spans in ((0, range(LEAD)), (1, range(PARTS)), (0, range(LEAD, PARTS))):
                if spans.start == 0:
                    pl.semaphore_wait(ready.at[(g + d) * TEAM + base + 2 * i], 1)
                for t in spans:
                    kv_copy(i, t, g + d, 1, cross_sem).start()

    def ask_both():
        for i, r in zip(pair, spot):
            @pl.when(r > place)
            def _():
                pl.semaphore_wait(ready.at[g * TEAM + base + 2 * i], 2)

            pl.when(r != place)(functools.partial(ask, i))

    pl.when(spot[1] < place)(ask_both)
    loop(1, teams, cross_back)
    pl.when(spot[1] >= place)(ask_both)
    for i, r in zip(pair, spot):
        pl.when(r != place)(functools.partial(near, i))

    @pl.when(c == 0)
    def _():
        pl.semaphore_wait(ready.at[me], 1)

    @pl.when(own)
    def _():
        for z in (qbuf.at[0], kvbuf.at[0]):
            pltpu.make_async_copy(z, z, load_sem.at[1]).wait()
        for t in range(PARTS):
            share(me, t).start()

    loop(1, teams, cross_on)

    maxima[...] = jnp.full_like(maxima, FLOOR)
    sums[...] = jnp.zeros_like(sums)
    accum[...] = jnp.zeros_like(accum)
    order_copy.wait()

    row = lax.broadcasted_iota(jnp.int32, (rows, rows), 0)
    col = lax.broadcasted_iota(jnp.int32, (rows, rows), 1)
    per = order.shape[0] // n
    blk = rows // per

    def placed(index, s):
        out = index + order[s * per] * blk
        for b in range(1, per):
            out = jnp.where(index >= b * blk, index + (order[s * per + b] - b) * blk, out)
        return out

    query_pos = [placed(row, g * TEAM + base + 2 * rs) for rs in range(2)]

    def fold(z):
        return z.reshape(rows, head_dim)

    def attend(parts, slots):
        for rs in parts:
            scores = []
            for slot in slots:
                one = lax.dot_general(
                    qbuf[rs], fold(kvbuf[slot, :, 0]), (((1,), (1,)), ((), ())),
                    preferred_element_type=jnp.float32) * scale
                allowed = placed(col, slot) <= query_pos[rs]
                scores.append(jnp.where(jnp.concatenate([allowed] * group, 0), one, MASKED))
            before = maxima[rs]
            top = functools.reduce(jnp.maximum, scores)
            fresh = jnp.maximum(before, jnp.max(top, axis=1, keepdims=True))
            factor = jnp.exp(before - fresh)
            maxima[rs] = fresh
            weights = [jnp.exp(one - fresh) for one in scores]
            sums[rs] = sums[rs] * factor + functools.reduce(jnp.add, weights)
            update = [
                lax.dot_general(
                    w.astype(jnp.bfloat16), fold(kvbuf[slot, :, 1]), (((1,), (0,)), ((), ())),
                    preferred_element_type=jnp.float32)
                for w, slot in zip(weights, slots)]
            accum[rs] = accum[rs] * jnp.concatenate(
                [factor] * (head_dim // rows), 1) + functools.reduce(jnp.add, update)

    def landed(slot, t):
        share(slot, t).wait_recv()

    def take(slot):
        for t in range(PARTS):
            landed(slot, t)

            @pl.when(c == 1)
            def _():
                share(slot, t).start()
        return slot

    @pl.when(other)
    def _():
        for t in range(PARTS):
            landed(me, t)

    for rs in range(2):
        @pl.when(other | (upper != rs))
        def _():
            pltpu.make_async_remote_copy(
                src_ref=qout.at[0], dst_ref=qbuf.at[rs], send_sem=q_send,
                recv_sem=q_recv.at[rs], device_id=(me, partner), device_id_type=MESH).wait_recv()

    attend((0, 1), (me,))

    beside = g * TEAM + j + 1 - 2 * y
    above = g * TEAM + lax.rem(j + 2, TEAM)
    across = above + 1 - 2 * y
    for m in range(TEAM):
        @pl.when((m % 2 == c) & (rank(m) > place))
        def _():
            pl.semaphore_wait(ready.at[g * TEAM + m], 2)

    for xx in range(planes):
        @pl.when(xx < x)
        def _():
            signal(plane_ready, me, xx * 2 + c)

    both = (0, 1)
    if teams == 2:
        there = (1 - g) * TEAM
        close = (above, across)
        lead = 2 * upper
        far = [there + lead, there + lead + 1, there + 2 - lead, there + 3 - lead]


        attend(both, (take(beside),))
        low, up = g == 0, upper == 1
        stages = [
            (jnp.where(low & up, a, b),
             jnp.where(low & up, b, jnp.where(low | up, d, a)),
             jnp.where(low == up, d, a))
            for a, b, d in zip(close, far[:2], far[2:])]
        first, second, final = zip(*stages)
        attend(both, [take(s) for s in first])
        wait(plane_ready, planes - 1 - x)

        for xx in range(planes):
            @pl.when(xx > x)
            def _():
                signal(plane_ready, me, xx * 2 + c)

        attend(both, [take(s) for s in second])
        for s in final:
            take(s)
    else:
        attend(both, [take(s) for s in (beside, above, across)])
        wait(plane_ready, planes - 1 - x)

        for xx in range(planes):
            @pl.when(xx > x)
            def _():
                signal(plane_ready, me, xx * 2 + c)

        def slot_of(k):
            return lax.rem(g + 1 + k // TEAM, teams) * TEAM + lax.rem(k, TEAM)

        def further(k):
            attend(both, (take(slot_of(jnp.int32(k))),))

        loop(0, TEAM * (teams - 1) - 1, further)
        final = [slot_of(jnp.int32(TEAM * (teams - 1) - 1))]
        take(final[0])

    def finish(rs):
        total = jnp.sum(sums[rs], axis=1, keepdims=True)
        out = (accum[rs] * (1.0 / total)).astype(jnp.bfloat16)
        for g2 in range(group):
            obuf[rs, :, g2 * head_dim:(g2 + 1) * head_dim] = out[g2 * rows:(g2 + 1) * rows]
        return jnp.log(total) + maxima[rs]

    columns = lanes(((x * 2 + keeper) * 2 + upper) * width, width)
    wait(plane_ready, x)

    def send_out(rs, k):
        mine = own & (upper == rs)
        to = lax.rem(x + 1 + k, planes) * 2 + lax.rem(c + 1 + k // planes, 2)
        src = obuf.at[rs, pl.ds(pl.multiple_of(to * keep, keep), keep)]

        def away():
            pltpu.make_async_remote_copy(
                src_ref=src, dst_ref=attn.at[:, columns], send_sem=o_send, recv_sem=o_recv,
                device_id=(g * TEAM + base + 2 * rs, to), device_id_type=MESH).start()

        if k < nh - 1:
            away()
        else:
            pl.when(jnp.logical_not(mine))(away)

            @pl.when(mine)
            def _():
                pltpu.make_async_copy(src, attn.at[:, columns], o_send).start()

    def send_lse(rs, full):
        for g2 in range(group):
            lse_tx[rs, g2:g2 + 1, :] = jnp.transpose(full[g2 * rows:(g2 + 1) * rows])[:1]
        mine = own & (upper == rs)

        @pl.when(jnp.logical_not(mine))
        def _():
            pltpu.make_async_remote_copy(
                src_ref=lse_tx.at[rs], dst_ref=lse_rx.at[upper], send_sem=l_send, recv_sem=l_recv,
                device_id=(g * TEAM + base + 2 * rs, x * 2 + keeper), device_id_type=MESH).start()

        @pl.when(mine)
        def _():
            lse_rx[rs] = lse_tx[rs]

    attend(both, final)
    for rs in (1 - upper, upper):
        full = finish(rs)
        for k in range(nh):
            send_out(rs, k)
        send_lse(rs, full)

    def drain(ref, sem):
        pltpu.make_async_copy(ref, ref, sem).wait()

    def by_kind(ref, less, sem):
        pl.when(own)(lambda: drain(less, sem))
        pl.when(other)(lambda: drain(ref, sem))

    by_kind(lse_rx, lse_rx.at[pl.ds(0, 1)], l_recv)
    lse[...] = jnp.concatenate([lse_rx[0, :group], lse_rx[1, :group]], 0)
    by_kind(attn, attn.at[:, pl.ds(0, (2 * nh - 1) * width)], o_recv)
    drain(attn, o_send)
    by_kind(lse_tx, lse_tx.at[pl.ds(0, 1)], l_send)
    by_kind(qbuf, qbuf.at[pl.ds(0, 1)], q_send)
    by_kind(kvbuf.at[pl.ds(0, 2)], kvbuf.at[pl.ds(0, 1)], near_sem)
    drain(kvbuf.at[pl.ds(0, 2 * (teams - 1))], cross_sem)
    pl.when((c == 1) & own)(functools.partial(drain, kvbuf, share_sem))
    pl.when((c == 1) & other)(functools.partial(drain, kvbuf.at[pl.ds(0, n - 1)], share_sem))
    pl.when((c == 0) & own)(functools.partial(drain, kvbuf.at[0], share_sem))


def hand_over(attn, lse, attn_hbm, lse_hbm, sem):
    step = attn.shape[1] // 4
    copies = [pltpu.make_async_copy(lse, lse_hbm, sem.at[0])]
    for i in range(4):
        part = (slice(None), pl.ds(i * step, step))
        copies.append(pltpu.make_async_copy(attn.at[part], attn_hbm.at[part], sem.at[1 + i]))
    for c in copies:
        c.start()
    for c in copies:
        c.wait()


def local(n, nh, queries, keys, values, block_order):
    rows = queries.shape[0]
    head_dim, group = HEAD_SIZE, QUERY_GROUP
    high = group * rows
    bf16, f32 = jnp.bfloat16, jnp.float32
    dma = pltpu.SemaphoreType.DMA
    attn, lse = pl.pallas_call(
        functools.partial(kernel, n, nh),
        out_shape=(
            pltpu.VMEM((rows // nh, queries.shape[1] * nh), bf16),
            pltpu.VMEM((2 * group, rows), f32),
        ),
        in_specs=[pl.BlockSpec(memory_space=pl.ANY)] * 4,
        out_specs=(pl.BlockSpec(memory_space=pltpu.VMEM),) * 2,
        scratch_shapes=[
            pltpu.VMEM((2, high, head_dim), bf16),
            pltpu.VMEM((2, high, head_dim), bf16),
            pltpu.VMEM((2, PARTS, 2, rows // PARTS, head_dim), bf16),
            pltpu.VMEM((n, PARTS, 2, rows // PARTS, head_dim), bf16),
            pltpu.VMEM((2, high, rows), f32),
            pltpu.VMEM((2, high, rows), f32),
            pltpu.VMEM((2, high, head_dim), f32),
            pltpu.VMEM((2, rows, group * head_dim), bf16),
            pltpu.VMEM((2, 8, rows), f32),
            pltpu.VMEM((2, 8, rows), f32),
            pltpu.SMEM(block_order.shape, jnp.int32),
            dma((3,)),
            dma,
            dma,
            dma,
            dma((n, PARTS)),
            dma,
            dma((2,)),
            dma,
            dma,
            dma,
            dma,
            pltpu.SemaphoreType.REGULAR((n,)),
            pltpu.SemaphoreType.REGULAR,
        ],
        compiler_params=pltpu.CompilerParams(collective_id=0, has_side_effects=True),
    )(block_order, queries, keys, values)
    attn, lse = (pltpu.with_memory_space_constraint(z, pltpu.VMEM) for z in (attn, lse))
    return pl.pallas_call(
        hand_over,
        out_shape=(pltpu.HBM(attn.shape, bf16), pltpu.HBM(lse.shape, f32)),
        in_specs=[pl.BlockSpec(memory_space=pltpu.VMEM)] * 2,
        out_specs=(pl.BlockSpec(memory_space=pltpu.HBM),) * 2,
        scratch_shapes=[dma((5,))],
    )(attn, lse)


def solution(mesh):
    in_specs = (P("seq", "head"), P("seq", "head"), P("seq", "head"), P())
    out_specs = (P(("seq", "head"), None), P("head", "seq"))
    body = functools.partial(local, mesh.shape["seq"], mesh.shape["head"])
    return jax.shard_map(body, mesh=mesh, in_specs=in_specs, out_specs=out_specs, check_vma=False)
```
